32 devices in a mesh: dp: 1 (over z), ep: 32 (over y, x, core).
Axes of the slice: x: 4, y: 4, z: 1, core: 2. Of those that a mesh axis runs over, the one named last changes fastest.
The devices are a block of a 4x4x8 slice.
Arguments:
- resid_in: bfloat16 [4096, 2048], P(('dp', 'ep'))
- expert_ids: int32 [4096, 6], P(('dp', 'ep'))
- priority: int32 [4096, 6], P(('dp', 'ep'))
- norm_gain: float32 [2048], replicated
- router_w: bfloat16 [2048, 64], replicated
- shared_w1: bfloat16 [2048, 2816], replicated
- shared_w3: bfloat16 [2048, 2816], replicated
- shared_w2: bfloat16 [2816, 2048], replicated
- expert_w1: bfloat16 [64, 2048, 1408], P('ep')
- expert_w3: bfloat16 [64, 2048, 1408], P('ep')
- expert_w2: bfloat16 [64, 1408, 2048], P('ep')
Outputs:
- output: bfloat16 [4096, 2048], P(('dp', 'ep'))
All inputs are finite; a program needn't handle non-finite values.
Results may differ from the reference program's by a relative error of at most 0.00677691.
Values are sent between devices in bfloat16 or wider.
A program may use at most 768 MiB of HBM per device.

```python
import math
import jax
import jax.numpy as jnp
from jax import lax

HIDDEN = 2048
EXPERTS = 64
TOP_K = 6
EXPERT_FF = 1408
SHARED_FF = 2816
GROUPS = 1
TOP_GROUPS = 1
EP_SIZE = 32
TOKENS = 4096
CAPACITY = 768

NORM_EPS = 1e-6
ROUTE_SCALE = 16.0


def draw_routing(route_key):
    key_group, key_score, key_hot, key_prio = jax.random.split(route_key, 4)
    group_width = EXPERTS // GROUPS
    n_cand = TOP_GROUPS * group_width
    local_experts = EXPERTS // EP_SIZE
    hot_range = 1280 * TOP_K // n_cand
    hot_dev = jax.random.permutation(key_hot, EP_SIZE) * hot_range // EP_SIZE
    group_score = jax.random.randint(key_group, (TOKENS, GROUPS), 0, 1 << 20) * GROUPS + jnp.arange(GROUPS)
    group_pick = lax.top_k(group_score, TOP_GROUPS)[1]
    cand_ids = (group_pick[:, :, None] * group_width + jnp.arange(group_width)).reshape(TOKENS, n_cand)
    score_noise = jax.random.randint(key_score, (TOKENS, n_cand), 0, 1024)
    cand_score = (score_noise + hot_dev[cand_ids // local_experts]) * n_cand + jnp.arange(n_cand)
    pick_idx = lax.top_k(cand_score, TOP_K)[1]
    expert_ids = jnp.take_along_axis(cand_ids, pick_idx, axis=1).astype(jnp.int32)
    priority = jax.random.permutation(key_prio, TOKENS * TOP_K).reshape(TOKENS, TOP_K).astype(jnp.int32)
    return expert_ids, priority


def setup_inputs(seed: int = 0, part: int = 0) -> dict:
    root_key = jax.random.key(seed)
    resid_key, route_key = jax.random.split(jax.random.fold_in(root_key, part))
    weight_keys = jax.random.split(jax.random.fold_in(root_key, 1 << 30), 8)
    expert_ids, priority = draw_routing(route_key)
    down_gain = EXPERTS / (10.0 * math.sqrt(TOP_K))
    return dict(
        resid_in=jax.random.normal(resid_key, (TOKENS, HIDDEN), jnp.float32).astype(jnp.bfloat16),
        expert_ids=expert_ids,
        priority=priority,
        norm_gain=1.0 + 0.3 * jax.random.normal(weight_keys[0], (HIDDEN,), jnp.float32),
        router_w=(0.5 * HIDDEN ** -0.5 * jax.random.normal(weight_keys[1], (HIDDEN, EXPERTS), jnp.float32)).astype(jnp.bfloat16),
        shared_w1=(HIDDEN ** -0.5 * jax.random.normal(weight_keys[2], (HIDDEN, SHARED_FF), jnp.float32)).astype(jnp.bfloat16),
        shared_w3=(HIDDEN ** -0.5 * jax.random.normal(weight_keys[3], (HIDDEN, SHARED_FF), jnp.float32)).astype(jnp.bfloat16),
        shared_w2=(SHARED_FF ** -0.5 * jax.random.normal(weight_keys[4], (SHARED_FF, HIDDEN), jnp.float32)).astype(jnp.bfloat16),
        expert_w1=(HIDDEN ** -0.5 * jax.random.normal(weight_keys[5], (EXPERTS, HIDDEN, EXPERT_FF), jnp.float32)).astype(jnp.bfloat16),
        expert_w3=(HIDDEN ** -0.5 * jax.random.normal(weight_keys[6], (EXPERTS, HIDDEN, EXPERT_FF), jnp.float32)).astype(jnp.bfloat16),
        expert_w2=(down_gain * EXPERT_FF ** -0.5 * jax.random.normal(weight_keys[7], (EXPERTS, EXPERT_FF, HIDDEN), jnp.float32)).astype(jnp.bfloat16),
    )


def swiglu_ffn(normed, w_gate, w_up, w_down):
    up_a = jnp.dot(normed, w_gate, preferred_element_type=jnp.float32)
    up_b = jnp.dot(normed, w_up, preferred_element_type=jnp.float32)
    hidden_act = (jax.nn.silu(up_a) * up_b).astype(jnp.bfloat16)
    return jnp.dot(hidden_act, w_down, preferred_element_type=jnp.float32).astype(jnp.bfloat16)


def keep_mask(expert_ids, priority):
    n_assign = TOKENS * TOP_K
    owners = (expert_ids // (EXPERTS // EP_SIZE)).reshape(n_assign)
    prio_flat = priority.reshape(n_assign)
    owner_by_rank = jnp.zeros((n_assign,), jnp.int32).at[prio_flat].set(owners)
    dest_hits = (owner_by_rank[:, None] == jnp.arange(EP_SIZE, dtype=jnp.int32)).astype(jnp.int32)
    before = jnp.cumsum(dest_hits, axis=0) - dest_hits
    rank_by_prio = jnp.sum(before * dest_hits, axis=1)
    return (rank_by_prio[prio_flat] < CAPACITY).reshape(TOKENS, TOP_K)


def routed_sum(normed, expert_ids, flat_gates, expert_w1, expert_w3, expert_w2):
    n_assign = TOKENS * TOP_K
    row_block = max(8, n_assign // (32 * EXPERTS) * 8)
    n_blocks = n_assign // row_block + EXPERTS + 1
    flat_ids = expert_ids.reshape(n_assign)
    sort_order = jnp.argsort(flat_ids * n_assign + jnp.arange(n_assign, dtype=jnp.int32)).astype(jnp.int32)
    counts = jax.ops.segment_sum(jnp.ones((n_assign,), jnp.int32), flat_ids, num_segments=EXPERTS)
    padded = (counts + row_block - 1) // row_block * row_block
    pad_start = jnp.cumsum(padded) - padded
    sort_start = jnp.cumsum(counts) - counts
    sorted_ids = flat_ids[sort_order]
    dest_row = pad_start[sorted_ids] + jnp.arange(n_assign, dtype=jnp.int32) - sort_start[sorted_ids]
    row_src = jnp.full((n_blocks * row_block,), n_assign, jnp.int32).at[dest_row].set(sort_order)
    block_first = jnp.arange(n_blocks, dtype=jnp.int32) * row_block
    block_expert = jnp.sum((pad_start[None, :] <= block_first[:, None]).astype(jnp.int32), axis=1) - 1
    normed_pad = jnp.concatenate([normed, jnp.zeros((1, HIDDEN), normed.dtype)], axis=0)
    gates_pad = jnp.concatenate([flat_gates, jnp.zeros((1,), flat_gates.dtype)])

    def one_block(routed_acc, block_args):
        src_rows, expert = block_args
        tok_rows = src_rows // TOP_K
        expert_out = swiglu_ffn(normed_pad[tok_rows], expert_w1[expert], expert_w3[expert], expert_w2[expert])
        weighted = expert_out.astype(jnp.float32) * gates_pad[src_rows][:, None]
        return routed_acc.at[tok_rows].add(weighted), None

    routed_acc = lax.scan(one_block, jnp.zeros((TOKENS + 1, HIDDEN), jnp.float32), (row_src.reshape(n_blocks, row_block), block_expert))[0]
    return routed_acc[:TOKENS]


def reference(resid_in, expert_ids, priority, norm_gain, router_w, shared_w1, shared_w3, shared_w2, expert_w1, expert_w3, expert_w2):
    resid32 = resid_in.astype(jnp.float32)
    inv_rms = lax.rsqrt(jnp.mean(resid32 * resid32, axis=1, keepdims=True) + NORM_EPS)
    normed = (resid32 * inv_rms * norm_gain).astype(jnp.bfloat16)
    gate_probs = jax.nn.softmax(jnp.dot(normed, router_w, preferred_element_type=jnp.float32), axis=1)
    gate_vals = ROUTE_SCALE * jnp.take_along_axis(gate_probs, expert_ids, axis=1)
    kept_mask = keep_mask(expert_ids, priority)
    flat_gates = jnp.where(kept_mask, gate_vals, 0.0).reshape(TOKENS * TOP_K)
    shared_out = swiglu_ffn(normed, shared_w1, shared_w3, shared_w2)
    routed = routed_sum(normed, expert_ids, flat_gates, expert_w1, expert_w3, expert_w2)
    return (resid32 + shared_out.astype(jnp.float32) + routed).astype(jnp.bfloat16)
```

```python
import functools
import math

import jax
import jax.numpy as jnp
from jax import lax
from jax.experimental import pallas as pl
from jax.experimental.pallas import tpu as pltpu
from jax.sharding import PartitionSpec as P

NORM_EPS = 1e-6
ROUTE_SCALE = 16.0
MESH = pl.DeviceIdType.MESH
F32 = jnp.float32
BF16 = jnp.bfloat16
FAR = 1 << 20
TILE = 128
CAP = 72
VMEM_LIMIT = 64000 * 1024


def rms_norm(resid_in, norm_gain):
    resid32 = resid_in.astype(F32)
    inv_rms = lax.rsqrt(jnp.mean(resid32 * resid32, axis=1, keepdims=True) + NORM_EPS)
    return (resid32 * inv_rms * norm_gain).astype(BF16)


def swiglu_ffn(normed, w_gate, w_up, w_down):
    up_a = jnp.dot(normed, w_gate, preferred_element_type=F32)
    up_b = jnp.dot(normed, w_up, preferred_element_type=F32)
    hidden_act = (jax.nn.silu(up_a) * up_b).astype(BF16)
    return jnp.dot(hidden_act, w_down, preferred_element_type=F32).astype(BF16)


class Place:
    def __init__(self, ep):
        self.side = math.isqrt(ep // 2)
        self.me = lax.axis_index("ep")
        self.core = lax.rem(self.me, 2)
        self.chip = self.me // 2
        self.px = lax.rem(self.chip, self.side)
        self.py = self.chip // self.side
        self.partner = self.me + 1 - 2 * self.core

    def dev(self, dx, dy, core=None):
        x = lax.rem(self.px + dx % self.side, self.side)
        y = lax.rem(self.py + dy % self.side, self.side)
        return (y * self.side + x) * 2 + (self.core if core is None else core)

    def at(self, fam, du, dv, core=None):
        return self.dev(du, dv, core) if fam == 0 else self.dev(dv, du, core)


def tri(n, m, rows_first):
    i = lax.broadcasted_iota(jnp.int32, (n, m), 0)
    j = lax.broadcasted_iota(jnp.int32, (n, m), 1)
    return jnp.where(i < j if rows_first else j < i, 1.0, 0.0).astype(BF16)


def mm(a, b):
    return jnp.dot(a.astype(BF16), b.astype(BF16), preferred_element_type=F32)


def route(pc, ep, top_k, n_local, n_chips, meta_all, ids, prs, pr, thr, cnt, kch, pos, ka, kb, info_ref, q_ref, mx_ref):
    n_exp = ep * n_local
    tok = ids.shape[2]
    capacity = tok * top_k
    n_bits = (ep * capacity).bit_length()

    def unpack(s, _):
        for k in range(top_k):
            ids[k, pl.ds(s, 1), :] = meta_all[s, k : k + 1, :]
            prs[k, pl.ds(s, 1), :] = meta_all[s, 8 + k : 9 + k, :]
        return 0

    lax.fori_loop(0, ep, unpack, 0)

    def per_expert(e, _):
        best = jnp.full((ep, tok), FAR, jnp.int32)
        for k in range(top_k):
            best = jnp.minimum(best, jnp.where(ids[k] == e, prs[k], FAR))
        pr[e] = best
        return 0

    lax.fori_loop(0, n_exp, per_expert, 0)

    thr[...] = jnp.zeros(thr.shape, jnp.int32)

    def bit_step(i, step):
        for d in range(ep):
            cand = thr[d : d + 1, :] + step
            hits = jnp.zeros((ep, tok), F32)
            for l in range(n_local):
                hits = hits + jnp.where(pr[d * n_local + l] < cand, 1.0, 0.0)
            cnt[d : d + 1, :] = jnp.sum(hits, axis=0, keepdims=True)
        total = jnp.sum(cnt[...], axis=1, keepdims=True)
        thr[...] = thr[...] + jnp.where(total <= capacity, step, 0)
        return step // 2

    lax.fori_loop(0, n_bits, bit_step, jnp.int32(1 << (n_bits - 1)))

    def chip_counts(d, _):
        kept = jnp.zeros((ep, tok), F32)
        for l in range(n_local):
            kept = kept + jnp.where(pr[d * n_local + l] < thr[pl.ds(d, 1), :], 1.0, 0.0)
        kch[pl.ds(pl.multiple_of(d * ep, ep), ep), :] = kept
        return 0

    lax.fori_loop(0, ep, chip_counts, 0)
    pairs = kch[pl.ds(0, ep * n_chips, stride=2), :] + kch[pl.ds(1, ep * n_chips, stride=2), :]
    worst = jnp.max(jnp.sum(pairs, axis=1, keepdims=True), axis=0, keepdims=True)
    mx_ref[...] = jnp.broadcast_to(worst, mx_ref.shape).astype(jnp.int32)

    upper = tri(tok, tok, True)
    ones = jnp.ones((tok, tok), BF16)
    lower = tri(ep, ep, False)
    my_thr = thr[pl.ds(pc.me, 1), :]
    base = jnp.zeros((1, tok), F32)
    for l in range(n_local):
        kept = pr[pc.me * n_local + l] < my_thr
        kept_f = jnp.where(kept, 1.0, 0.0)
        in_row = mm(kept_f, upper)
        row_total = mm(kept_f, ones)
        row_start = mm(lower, row_total)
        pos[l] = jnp.where(kept, (in_row + row_start + base), -1.0).astype(jnp.int32)
        info_ref[2 * l] = row_total.astype(jnp.int32)
        info_ref[2 * l + 1] = (row_start + base).astype(jnp.int32)
        group = jnp.sum(row_total, axis=0, keepdims=True)
        base = base + jnp.floor((group + (TILE - 1)) * (1.0 / TILE)) * TILE

    def chip_rows(e, _):
        limit = thr[pl.ds(e // n_local, 1), :]
        first = pr[e, pl.ds(pc.chip * 2, 1), :]
        second = pr[e, pl.ds(pc.chip * 2 + 1, 1), :]
        ka[pl.ds(e, 1), :] = jnp.where(first < limit, 1.0, 0.0)
        kb[pl.ds(e, 1), :] = jnp.where(second < limit, 1.0, 0.0)
        return 0

    lax.fori_loop(0, n_exp, chip_rows, 0)
    k_a, k_b = ka[...], kb[...]
    tot_a = mm(k_a, ones)
    both = tot_a + mm(k_b, ones)
    i = lax.broadcasted_iota(jnp.int32, (n_exp, n_exp), 0)
    j = lax.broadcasted_iota(jnp.int32, (n_exp, n_exp), 1)
    earlier = jnp.where((j < i) & (j // n_local == i // n_local), 1.0, 0.0)
    before = mm(earlier, both)
    q_a = jnp.where(k_a > 0, mm(k_a, upper) + before, -1.0)
    q_b = jnp.where(k_b > 0, mm(k_b, upper) + tot_a + before, -1.0)
    second_core = lax.broadcasted_iota(jnp.int32, q_ref.shape, 0) * 0 + pc.core
    q_ref[...] = jnp.where(second_core == 0, q_a, q_b).astype(jnp.int32)


def dispatch_kernel(
    ep, top_k, n_local, b_ref, meta_ref, x_ref, info_ref, q_ref, mx_ref, yall, meta_all, ids, prs, pr, thr, cnt, kch, pos, ka, kb,
    sel, own_sem, m_send, m_recv, s_send, s_recv, p_send, p_recv, o_send, o_recv,
):
    pc = Place(ep)
    side, me = pc.side, pc.me
    tok, dim = b_ref.shape
    half, quarter = tok // 2, tok // 4

    barrier = pltpu.get_barrier_semaphore()

    def greet(o, _):
        pl.semaphore_signal(barrier, inc=1, device_id={"ep": lax.rem(me + o, ep)}, device_id_type=MESH)
        return 0

    lax.fori_loop(1, ep, greet, 0)
    pl.semaphore_wait(barrier, ep - 1)

    own = pltpu.make_async_copy(b_ref, yall.at[me], own_sem)
    own.start()

    def meta_copy(o, src):
        return pltpu.make_async_remote_copy(
            src_ref=meta_ref, dst_ref=meta_all.at[src], send_sem=m_send.at[o], recv_sem=m_recv.at[o],
            device_id={"ep": lax.rem(me + o, ep)}, device_id_type=MESH,
        )

    def send_meta(o, _):
        meta_copy(o, me).start()
        return 0

    lax.fori_loop(1, ep, send_meta, 0)

    def piece(fam, g, k, sent):
        j = g - 1
        hop = {0: 1, 1: -1, 2: 1, 3: -1}[k]
        dist = {0: 0 if sent else -1, 1: 0 if sent else 1, 2: -1 if sent else 2, 3: 1 if sent else 2}[k]
        du, dv = (dist, 0) if g == 0 else (j, dist)
        start = fam * half + (quarter if k == 3 else 0)
        size = half if k < 2 else quarter
        return du % side, dv % side, start, size, hop

    def link_copy(fam, g, k, sent):
        du, dv, start, size, hop = piece(fam, g, k, sent)
        block = pc.at(fam, du, dv)
        rows = yall.at[block, pl.ds(start, size), :]
        source = b_ref.at[pl.ds(start, size), :] if sent and (du, dv) == (0, 0) else rows
        target = pc.at(fam, hop, 0) if g == 0 else pc.at(fam, 0, hop)
        n = (fam * (side + 1) + g) * 4 + k
        return pltpu.make_async_remote_copy(
            src_ref=source, dst_ref=rows, send_sem=s_send.at[n], recv_sem=s_recv.at[n], device_id={"ep": target}, device_id_type=MESH
        )

    def pass_on(fam, g, k, mine):
        du, dv, start, size, _ = piece(fam, g, k, False)
        block = pc.at(fam, du, dv, pc.core if mine else 1 - pc.core)
        rows = yall.at[block, pl.ds(start, size), :]
        n = (fam * (side + 1) + g) * 4 + k
        return pltpu.make_async_remote_copy(
            src_ref=rows, dst_ref=rows, send_sem=p_send.at[n], recv_sem=p_recv.at[n], device_id={"ep": pc.partner}, device_id_type=MESH
        )

    def own_to_partner(block):
        return pltpu.make_async_remote_copy(
            src_ref=b_ref, dst_ref=yall.at[block], send_sem=o_send, recv_sem=o_recv, device_id={"ep": pc.partner}, device_id_type=MESH
        )

    for fam in range(2):
        for k in range(2):
            link_copy(fam, 0, k, True).start()
    own_to_partner(me).start()
    for fam in range(2):
        for k in range(2):
            link_copy(fam, 1, k, True).start()

    def wait_meta(o, _):
        meta_copy(o, lax.rem(me - o + ep, ep)).wait_recv()
        return 0

    meta_all[me] = meta_ref[...]
    lax.fori_loop(1, ep, wait_meta, 0)
    route(pc, ep, top_k, n_local, ep // 2, meta_all, ids, prs, pr, thr, cnt, kch, pos, ka, kb, info_ref, q_ref, mx_ref)

    slots = x_ref.shape[0]
    n_cols = 256
    started = []

    def pick(chips):
        blocks = [pc.dev(dx, dy, core) for dx, dy in chips for core in range(2)]

        def build(i, _):
            rows = pl.ds(pl.multiple_of(i * TILE, TILE), TILE)
            slot = lax.broadcasted_iota(jnp.int32, (TILE, tok), 0) + i * TILE
            for n, block in enumerate(blocks):
                hit = slot == pos[0, pl.ds(block, 1), :]
                for l in range(1, n_local):
                    hit = hit | (slot == pos[l, pl.ds(block, 1), :])
                sel[rows, n * tok : (n + 1) * tok] = jnp.where(hit, 1.0, 0.0).astype(BF16)
            return 0

        lax.fori_loop(0, slots // TILE, build, 0)
        first = not started
        started.append(chips)

        def one(n, _):
            cols = pl.ds(pl.multiple_of(n * n_cols, n_cols), n_cols)
            source = jnp.concatenate([yall[block, :, cols] for block in blocks], axis=0)
            picked = jnp.dot(sel[...], source, preferred_element_type=F32).astype(BF16)
            x_ref[:, cols] = picked if first else x_ref[:, cols] + picked
            return 0

        lax.fori_loop(0, dim // n_cols, one, 0)

    order = [(f, 0, k) for f in range(2) for k in range(2)]
    order += [(f, 1, k) for f in range(2) for k in range(2)]
    order += [(f, 0, k) for f in range(2) for k in (2, 3)]
    order += [(f, g, k) for g in (side, 2) for f in range(2) for k in range(2)]
    order += [(f, 1, k) for f in range(2) for k in (2, 3)]
    order += [(f, 3, k) for f in range(2) for k in range(2)]
    order += [(f, g, k) for g in (side, 2, 3) for f in range(2) for k in (2, 3)]

    def chip_of(fam, g, k):
        du, dv = piece(fam, g, k, False)[:2]
        return (du, dv) if fam == 0 else (dv, du)

    parts = {}
    for fam, g, k in order:
        parts[chip_of(fam, g, k)] = parts.get(chip_of(fam, g, k), 0) + 2

    complete = [(0, 0)]
    got = set()

    def landed(fam, g, k):
        chip = chip_of(fam, g, k)
        parts[chip] -= 1
        if parts[chip] == 0:
            complete.append(chip)

    own.wait()
    own_to_partner(pc.partner).wait_recv()
    lag = 4
    for i in range(len(order) + lag):
        if i < len(order):
            fam, g, k = order[i]
            link_copy(fam, g, k, False).wait_recv()
            got.add((fam, g, k))
            if k < 2:
                link_copy(fam, g, k + 2, True).start()
                if g == 0:
                    j = side - 1 if k == 0 else 1
                    for kk in range(2):
                        link_copy(fam, 1 + j, kk, True).start()
            elif g == 0 and (fam, g, 2) in got and (fam, g, 3) in got:
                for kk in range(2):
                    link_copy(fam, 3, kk, True).start()
            pass_on(fam, g, k, True).start()
            landed(fam, g, k)
        if i >= lag:
            fam, g, k = order[i - lag]
            pass_on(fam, g, k, False).wait_recv()
            landed(fam, g, k)
        while len(complete) >= 2:
            pick([complete.pop(0), complete.pop(0)])

    def sent_meta(o, _):
        meta_copy(o, me).wait_send()
        return 0

    lax.fori_loop(1, ep, sent_meta, 0)
    own_to_partner(me).wait_send()
    for fam, g, k in order:
        link_copy(fam, g, k, True).wait_send()
        pass_on(fam, g, k, True).wait_send()


def dispatch(ep, n_local, normed, expert_ids, priority):
    tok, dim = normed.shape
    top_k = expert_ids.shape[1]
    side = math.isqrt(ep // 2)
    n_exp = ep * n_local
    slots = tok * top_k + (n_local - 1) * TILE
    pad = jnp.zeros((8 - top_k, tok), jnp.int32)
    meta = jnp.concatenate([expert_ids.T, pad, priority.T, pad], axis=0)
    n_piece = 2 * (side + 1) * 4
    vmem = pl.BlockSpec(memory_space=pltpu.VMEM)
    dma = pltpu.SemaphoreType.DMA
    return pl.pallas_call(
        functools.partial(dispatch_kernel, ep, top_k, n_local),
        out_shape=(
            jax.ShapeDtypeStruct((slots, dim), BF16),
            jax.ShapeDtypeStruct((2 * n_local, ep, tok), jnp.int32),
            jax.ShapeDtypeStruct((n_exp, tok), jnp.int32),
            jax.ShapeDtypeStruct((8, 128), jnp.int32),
        ),
        in_specs=[vmem, vmem],
        out_specs=(vmem, vmem, vmem, vmem),
        scratch_shapes=[
            pltpu.VMEM((ep, tok, dim), BF16),
            pltpu.VMEM((ep, 16, tok), jnp.int32),
            pltpu.VMEM((top_k, ep, tok), jnp.int32),
            pltpu.VMEM((top_k, ep, tok), jnp.int32),
            pltpu.VMEM((n_exp, ep, tok), jnp.int32),
            pltpu.VMEM((ep, tok), jnp.int32),
            pltpu.VMEM((ep, tok), F32),
            pltpu.VMEM((ep * ep, tok), F32),
            pltpu.VMEM((n_local, ep, tok), jnp.int32),
            pltpu.VMEM((n_exp, tok), F32),
            pltpu.VMEM((n_exp, tok), F32),
            pltpu.VMEM((slots, 4 * tok), BF16),
            dma(()), dma((ep,)), dma((ep,)), dma((n_piece,)), dma((n_piece,)), dma((n_piece,)), dma((n_piece,)), dma(()), dma(()),
        ],
        compiler_params=pltpu.CompilerParams(collective_id=0, has_side_effects=True, vmem_limit_bytes=VMEM_LIMIT),
        name="dispatch",
    )(normed, meta)


def expert_kernel(sc, x_ref, w1_hbm, w3_hbm, w2_hbm, e_ref, w1, w3, w2, sems):
    n_local, ep = w1.shape[0], sc.shape[1]
    slots = x_ref.shape[0]
    loads = []
    for l in range(n_local):
        for n, (src, dst) in enumerate(((w1_hbm, w1), (w3_hbm, w3), (w2_hbm, w2))):
            loads.append(pltpu.make_async_copy(src.at[l], dst.at[l], sems.at[l, n]))
            loads[-1].start()
    tiles = [(sc[2 * l + 1, ep - 1] - sc[2 * l + 1, 0] + sc[2 * l, ep - 1] + TILE - 1) // TILE for l in range(n_local)]
    done = 0
    for l in range(n_local):
        loads[3 * l].wait()
        loads[3 * l + 1].wait()
        loads[3 * l + 2].wait()

        def one(i, _, l=l, done=done):
            rows = pl.ds(pl.multiple_of((done + i) * TILE, TILE), TILE)
            x = x_ref[rows, :]
            up_a = jnp.dot(x, w1[l], preferred_element_type=F32)
            up_b = jnp.dot(x, w3[l], preferred_element_type=F32)
            act = (up_a * jax.nn.sigmoid(up_a) * up_b).astype(BF16)
            e_ref[rows, :] = jnp.dot(act, w2[l], preferred_element_type=F32).astype(BF16)
            return 0

        lax.fori_loop(0, tiles[l], one, 0)
        done = done + tiles[l]

    def clear(i, _):
        rows = pl.ds(pl.multiple_of(i * TILE, TILE), TILE)
        e_ref[rows, :] = jnp.zeros((TILE, e_ref.shape[1]), BF16)
        return 0

    lax.fori_loop(done, slots // TILE, clear, 0)


def experts(scalars, x, expert_w1, expert_w3, expert_w2):
    vmem = pl.BlockSpec(memory_space=pltpu.VMEM)
    hbm = pl.BlockSpec(memory_space=pl.ANY)
    n_local, dim, ff = expert_w1.shape
    return pl.pallas_call(
        expert_kernel,
        out_shape=jax.ShapeDtypeStruct(x.shape, BF16),
        in_specs=[pl.BlockSpec(memory_space=pltpu.SMEM), vmem, hbm, hbm, hbm],
        out_specs=vmem,
        scratch_shapes=[
            pltpu.VMEM((n_local, dim, ff), BF16),
            pltpu.VMEM((n_local, dim, ff), BF16),
            pltpu.VMEM((n_local, ff, dim), BF16),
            pltpu.SemaphoreType.DMA((n_local, 3)),
        ],
        compiler_params=pltpu.CompilerParams(vmem_limit_bytes=VMEM_LIMIT),
        name="experts",
    )(scalars, x, expert_w1, expert_w3, expert_w2)


def fill_kernel(ep, sc, rnd, e_ref, a_ref, b_ref):
    pc = Place(ep)
    side = pc.side
    slots, dim = e_ref.shape
    n_local = sc.shape[0] // 2
    width = dim // 4
    window = (CAP + 15 + 15) // 16 * 16
    skip = rnd[0] * CAP

    def one(n, _):
        dx, dy = lax.rem(n, side), n // side
        chip = lax.rem(pc.py + dy, side) * side + lax.rem(pc.px + dx, side)
        row = lax.broadcasted_iota(jnp.int32, (CAP, window), 0)
        col = lax.broadcasted_iota(jnp.int32, (CAP, window), 1)
        picks, sources = [], []
        lead = -skip
        for l in range(n_local):
            start, count = sc[2 * l + 1, 2 * chip], sc[2 * l, 2 * chip] + sc[2 * l, 2 * chip + 1]
            used = jnp.minimum(jnp.maximum(-lead, 0), count)
            origin = jnp.minimum((start + used) // 16 * 16, slots - window)
            origin = pl.multiple_of(origin, 16)
            slot = row - lead + start
            hit = (slot == col + origin) & (row >= lead) & (row < lead + count)
            picks.append(jnp.where(hit, 1.0, 0.0).astype(BF16))
            sources.append(e_ref[pl.ds(origin, window), :])
            lead = lead + count
        out = jnp.dot(picks[0], sources[0], preferred_element_type=F32)
        for l in range(1, n_local):
            out = out + jnp.dot(picks[l], sources[l], preferred_element_type=F32)
        out = out.astype(BF16)
        for c in range(2):
            a_ref[dx, c, dy] = out[:, c * width : (c + 1) * width]
            b_ref[dy, c, dx] = out[:, (2 + c) * width : (3 + c) * width]
        return 0

    lax.fori_loop(0, side * side, one, 0)


def fill(ep, scalars, rnd, e):
    side = math.isqrt(ep // 2)
    vmem = pl.BlockSpec(memory_space=pltpu.VMEM)
    smem = pl.BlockSpec(memory_space=pltpu.SMEM)
    bucket = jax.ShapeDtypeStruct((side, 2, side, CAP, e.shape[1] // 4), BF16)
    return pl.pallas_call(
        functools.partial(fill_kernel, ep),
        out_shape=(bucket, bucket),
        in_specs=[smem, smem, vmem],
        out_specs=(vmem, vmem),
        compiler_params=pltpu.CompilerParams(vmem_limit_bytes=VMEM_LIMIT),
        name="fill",
    )(scalars, rnd, e)


def combine_kernel(
    ep, n_local, bka, bkb, q_ref, p_ref, acc_ref, out_ref, st, rl, fin, ry, pf, g_ref, s_send, s_recv, p_send, p_recv
):
    pc = Place(ep)
    side = pc.side
    tok = q_ref.shape[1]
    width = bka.shape[-1]
    bk = (bka, bkb)

    barrier = pltpu.get_barrier_semaphore()
    friends = [pc.dev(1, 0), pc.dev(-1, 0), pc.dev(0, 1), pc.dev(0, -1), pc.partner]
    for friend in friends:
        pl.semaphore_signal(barrier, inc=1, device_id={"ep": friend}, device_id_type=MESH)
    pl.semaphore_wait(barrier, len(friends))

    def held(fam, j):
        return bk[fam].at[0] if j == 0 else st.at[fam, j]

    def link_copy(fam, g, k):
        hop = 1 if k % 2 == 0 else -1
        c = k % 2
        if g == 0:
            target = pc.at(fam, hop, 0)
            if k < 2:
                src, dst = bk[fam].at[hop % side], st.at[fam, hop % side]
            elif k < 4:
                src, dst = bk[fam].at[2, c], rl.at[fam, c]
            else:
                src, dst = rl.at[fam, c], st.at[fam, 2, c]
        else:
            j = g - 1
            target = pc.at(fam, 0, hop)
            if k < 2:
                src, dst = held(fam, j).at[:, hop % side], fin.at[fam, j, hop % side]
            elif k < 4:
                src, dst = held(fam, j).at[c, 2], ry.at[fam, j, c]
            else:
                src, dst = ry.at[fam, j, c], fin.at[fam, j, 2, c]
        n = (fam * (side + 1) + g) * 6 + k
        return pltpu.make_async_remote_copy(
            src_ref=src, dst_ref=dst, send_sem=s_send.at[n], recv_sem=s_recv.at[n], device_id={"ep": target}, device_id_type=MESH
        )

    def arrived(fam, j, v):
        return held(fam, j).at[:, 0] if v == 0 else fin.at[fam, j, v]

    def pass_on(fam, j, v):
        n = (fam * side + j) * side + v
        return pltpu.make_async_remote_copy(
            src_ref=arrived(fam, j, v), dst_ref=pf.at[fam, j, v], send_sem=p_send.at[n], recv_sem=p_recv.at[n],
            device_id={"ep": pc.partner}, device_id_type=MESH,
        )

    for k in (2, 3, 0, 1):
        for fam in range(2):
            link_copy(fam, 0, k).start()
    for k in (2, 3, 0, 1):
        for fam in range(2):
            link_copy(fam, 1, k).start()
    for fam in range(2):
        pass_on(fam, 0, 0).start()

    row = lax.broadcasted_iota(jnp.int32, (g_ref.shape[3], tok), 0)

    def weights(d, _):
        w = jnp.zeros(row.shape, F32)
        for l in range(n_local):
            e = d * n_local + l
            w = w + jnp.where(row == q_ref[pl.ds(e, 1), :], p_ref[pl.ds(e, 1), :], 0.0)
        w = w.T
        for n in range(3):
            term = w.astype(BF16)
            g_ref[d, n] = term
            w = w - term.astype(F32)
        return 0

    lax.fori_loop(0, ep, weights, 0)
    out_ref[...] = acc_ref[...]

    def add(fam, j, v):
        devs = [pc.at(fam, -j, -v), pc.at(fam, -j, -v, 1 - pc.core)]
        for c in range(2):
            cols = slice((2 * fam + c) * width, (2 * fam + c + 1) * width)
            total = out_ref[:, cols]
            for d, rows in zip(devs, (arrived(fam, j, v), pf.at[fam, j, v])):
                data = rows[c]
                for n in range(3):
                    total = total + jnp.dot(g_ref[d, n][:, :CAP], data, preferred_element_type=F32)
            out_ref[:, cols] = total

    ready = []

    def here(fam, j, v):
        pass_on(fam, j, v).start()
        ready.append((fam, j, v))

    def drain(keep):
        while len(ready) > keep:
            fam, j, v = ready.pop(0)
            pass_on(fam, j, v).wait_recv()
            add(fam, j, v)

    def got(fam, g, k):
        link_copy(fam, g, k).wait_recv()

    ready += [(0, 0, 0), (1, 0, 0)]
    for k in (2, 3):
        for fam in range(2):
            got(fam, 0, k)
            link_copy(fam, 0, k + 2).start()
    drain(0)
    for k in (0, 1):
        for fam in range(2):
            got(fam, 0, k)
            j = 1 if k == 0 else side - 1
            for kk in (2, 3, 0, 1):
                link_copy(fam, 1 + j, kk).start()
            here(fam, j, 0)
    for k in (2, 3):
        for fam in range(2):
            got(fam, 1, k)
            link_copy(fam, 1, k + 2).start()
    for fam in range(2):
        got(fam, 0, 4)
        got(fam, 0, 5)
        for kk in (2, 3, 0, 1):
            link_copy(fam, 3, kk).start()
        here(fam, 2, 0)
    drain(2)
    for j in (0, 1, side - 1, 2):
        if j > 0:
            for k in (2, 3):
                for fam in range(2):
                    got(fam, 1 + j, k)
                    link_copy(fam, 1 + j, k + 2).start()
        for k in (0, 1):
            for fam in range(2):
                got(fam, 1 + j, k)
                here(fam, j, 1 if k == 0 else side - 1)
        drain(2)
    for j in (0, 1, side - 1, 2):
        for fam in range(2):
            got(fam, 1 + j, 4)
            got(fam, 1 + j, 5)
            here(fam, j, 2)
        drain(2)
    drain(0)
    for fam in range(2):
        for g in range(side + 1):
            for k in range(6):
                link_copy(fam, g, k).wait_send()
        for j in range(side):
            for v in range(side):
                pass_on(fam, j, v).wait_send()


def combine(ep, n_local, bka, bkb, q, weights, acc):
    side = math.isqrt(ep // 2)
    cap, width = bka.shape[-2:]
    tok = q.shape[1]
    vmem = pl.BlockSpec(memory_space=pltpu.VMEM)
    dma = pltpu.SemaphoreType.DMA
    n_link, n_pass = 2 * (side + 1) * 6, 2 * side * side
    return pl.pallas_call(
        functools.partial(combine_kernel, ep, n_local),
        out_shape=jax.ShapeDtypeStruct(acc.shape, F32),
        in_specs=[vmem] * 5,
        out_specs=vmem,
        scratch_shapes=[
            pltpu.VMEM((2, side, 2, side, cap, width), BF16),
            pltpu.VMEM((2, 2, side, cap, width), BF16),
            pltpu.VMEM((2, side, side, 2, cap, width), BF16),
            pltpu.VMEM((2, side, 2, cap, width), BF16),
            pltpu.VMEM((2, side, side, 2, cap, width), BF16),
            pltpu.VMEM((ep, 3, tok, tok), BF16),
            dma((n_link,)), dma((n_link,)), dma((n_pass,)), dma((n_pass,)),
        ],
        compiler_params=pltpu.CompilerParams(collective_id=1, has_side_effects=True, vmem_limit_bytes=VMEM_LIMIT),
        name="combine",
    )(bka, bkb, q, weights, acc)


def solution(mesh):
    ep = mesh.shape["ep"]
    tok_spec = P(("dp", "ep"))
    expert_spec = P("ep")

    def device_fn(resid_in, expert_ids, priority, norm_gain, router_w, shared_w1, shared_w3, shared_w2, expert_w1, expert_w3, expert_w2):
        n_local = expert_w1.shape[0]
        normed = rms_norm(resid_in, norm_gain)
        x, info, q, worst = dispatch(ep, n_local, normed, expert_ids, priority)
        gates = ROUTE_SCALE * jax.nn.softmax(jnp.dot(normed, router_w, preferred_element_type=F32), axis=1)
        shared_out = swiglu_ffn(normed, shared_w1, shared_w3, shared_w2)
        scalars = info[:, :, 0]
        e = experts(scalars, x, expert_w1, expert_w3, expert_w2)
        rounds = (worst[0, 0] + CAP - 1) // CAP
        gates_t = gates.T

        def one_round(carry):
            rnd, acc = carry
            bka, bkb = fill(ep, scalars, rnd[None], e)
            return rnd + 1, combine(ep, n_local, bka, bkb, q - rnd * CAP, gates_t, acc)

        start = (jnp.int32(0), jnp.zeros(resid_in.shape, F32))
        routed = lax.while_loop(lambda carry: (carry[0] == 0) | (carry[0] < rounds), one_round, start)[1]
        return (resid_in.astype(F32) + shared_out.astype(F32) + routed).astype(BF16)

    return jax.shard_map(
        device_fn, mesh=mesh,
        in_specs=(tok_spec, tok_spec, tok_spec, P(), P(), P(), P(), P(), expert_spec, expert_spec, expert_spec),
        out_specs=tok_spec, check_vma=False,
    )
```

```python
import functools
import math

import jax
import jax.numpy as jnp
from jax import lax
from jax.experimental import pallas as pl
from jax.experimental.pallas import tpu as pltpu
from jax.sharding import PartitionSpec as P

NORM_EPS = 1e-6
ROUTE_SCALE = 16.0
MESH = pl.DeviceIdType.MESH
F32 = jnp.float32
BF16 = jnp.bfloat16
FAR = 1 << 20
TILE = 128
CAP = 72
VMEM_LIMIT = 64000 * 1024


class Place:
    def __init__(self, ep):
        self.side = math.isqrt(ep // 2)
        self.me = lax.axis_index("ep")
        self.core = lax.rem(self.me, 2)
        self.chip = self.me // 2
        self.px = lax.rem(self.chip, self.side)
        self.py = self.chip // self.side
        self.partner = self.me + 1 - 2 * self.core

    def dev(self, dx, dy, core=None):
        x = lax.rem(self.px + dx % self.side, self.side)
        y = lax.rem(self.py + dy % self.side, self.side)
        return (y * self.side + x) * 2 + (self.core if core is None else core)

    def at(self, fam, du, dv, core=None):
        return self.dev(du, dv, core) if fam == 0 else self.dev(dv, du, core)


def tri(n, m, rows_first):
    i = lax.broadcasted_iota(jnp.int32, (n, m), 0)
    j = lax.broadcasted_iota(jnp.int32, (n, m), 1)
    return jnp.where(i < j if rows_first else j < i, 1.0, 0.0).astype(BF16)


def mm(a, b):
    return jnp.dot(a.astype(BF16), b.astype(BF16), preferred_element_type=F32)


def mm_t(a, b):
    return lax.dot_general(a.astype(BF16), b.astype(BF16), (((1,), (1,)), ((), ())), preferred_element_type=F32)


def route(pc, ep, top_k, n_local, n_chips, meta_all, ids, prs, pr, thr, cnt, kch, pos, ka, kb, info_ref, q_ref):
    n_exp = ep * n_local
    tok = ids.shape[2]
    capacity = tok * top_k
    n_bits = (ep * capacity).bit_length()

    def unpack(s, _):
        for k in range(top_k):
            ids[k, pl.ds(s, 1), :] = meta_all[s, k : k + 1, :]
            prs[k, pl.ds(s, 1), :] = meta_all[s, 8 + k : 9 + k, :]
        return 0

    lax.fori_loop(0, ep, unpack, 0)

    def per_expert(e, _):
        best = jnp.full((ep, tok), FAR, jnp.int32)
        for k in range(top_k):
            best = jnp.minimum(best, jnp.where(ids[k] == e, prs[k], FAR))
        pr[e] = best
        return 0

    lax.fori_loop(0, n_exp, per_expert, 0)

    thr[...] = jnp.zeros(thr.shape, jnp.int32)

    def bit_step(i, step):
        for d in range(ep):
            cand = thr[d : d + 1, :] + step
            hits = jnp.zeros((ep, tok), F32)
            for l in range(n_local):
                hits = hits + jnp.where(pr[d * n_local + l] < cand, 1.0, 0.0)
            cnt[d : d + 1, :] = jnp.sum(hits, axis=0, keepdims=True)
        total = jnp.sum(cnt[...], axis=1, keepdims=True)
        thr[...] = thr[...] + jnp.where(total <= capacity, step, 0)
        return step // 2

    lax.fori_loop(0, n_bits, bit_step, jnp.int32(1 << (n_bits - 1)))

    def chip_counts(d, _):
        kept = jnp.zeros((ep, tok), F32)
        for l in range(n_local):
            kept = kept + jnp.where(pr[d * n_local + l] < thr[pl.ds(d, 1), :], 1.0, 0.0)
        kch[pl.ds(pl.multiple_of(d * ep, ep), ep), :] = kept
        return 0

    lax.fori_loop(0, ep, chip_counts, 0)
    pairs = kch[pl.ds(0, ep * n_chips, stride=2), :] + kch[pl.ds(1, ep * n_chips, stride=2), :]
    worst = jnp.max(jnp.sum(pairs, axis=1, keepdims=True), axis=0, keepdims=True)
    info_ref[...] = jnp.broadcast_to(worst, info_ref.shape).astype(jnp.int32)
    upper = tri(tok, tok, True)
    ones = jnp.ones((tok, tok), BF16)
    lower = tri(ep, ep, False)
    my_thr = thr[pl.ds(pc.me, 1), :]
    base = jnp.zeros((1, tok), F32)
    for l in range(n_local):
        kept = pr[pc.me * n_local + l] < my_thr
        kept_f = jnp.where(kept, 1.0, 0.0)
        in_row = mm(kept_f, upper)
        row_total = mm(kept_f, ones)
        row_start = mm(lower, row_total)
        pos[l] = jnp.where(kept, (in_row + row_start + base), -1.0).astype(jnp.int32)
        totals = mm_t(jnp.ones((8, tok), F32), kept_f)
        starts = mm(totals, tri(ep, ep, True)) + base[:, :ep]
        info_ref[2 * l : 2 * l + 1, :ep] = totals[:1].astype(jnp.int32)
        info_ref[2 * l + 1 : 2 * l + 2, :ep] = starts[:1].astype(jnp.int32)
        group = jnp.sum(row_total, axis=0, keepdims=True)
        base = base + jnp.floor((group + (TILE - 1)) * (1.0 / TILE)) * TILE

    def chip_rows(e, _):
        limit = thr[pl.ds(e // n_local, 1), :]
        first = pr[e, pl.ds(pc.chip * 2, 1), :]
        second = pr[e, pl.ds(pc.chip * 2 + 1, 1), :]
        ka[pl.ds(e, 1), :] = jnp.where(first < limit, 1.0, 0.0)
        kb[pl.ds(e, 1), :] = jnp.where(second < limit, 1.0, 0.0)
        return 0

    lax.fori_loop(0, n_exp, chip_rows, 0)
    k_a, k_b = ka[...], kb[...]
    tot_a = mm(k_a, ones)
    both = tot_a + mm(k_b, ones)
    i = lax.broadcasted_iota(jnp.int32, (n_exp, n_exp), 0)
    j = lax.broadcasted_iota(jnp.int32, (n_exp, n_exp), 1)
    earlier = jnp.where((j < i) & (j // n_local == i // n_local), 1.0, 0.0)
    before = mm(earlier, both)
    q_a = jnp.where(k_a > 0, mm(k_a, upper) + before, -1.0)
    q_b = jnp.where(k_b > 0, mm(k_b, upper) + tot_a + before, -1.0)
    second_core = lax.broadcasted_iota(jnp.int32, q_ref.shape, 0) * 0 + pc.core
    q_ref[...] = jnp.where(second_core == 0, q_a, q_b).astype(jnp.int32)


def dispatch_kernel(
    ep, top_k, n_local, y_ref, ids_ref, prio_ref, gain_ref, router_ref, sw1_hbm, sw3_hbm, sw2_hbm,
    x_hbm, info_ref, q_ref, gate_ref, base_ref,
    x_ref, b_ref, meta_ref, yall, meta_all, ids, prs, pr, thr, cnt, kch, pos, ka, kb, sel, sw1, sw3, sw2,
    own_sem, x_sem, sw_sem, m_send, m_recv, s_send, s_recv, p_send, p_recv, o_send, o_recv,
):
    pc = Place(ep)
    side, me = pc.side, pc.me
    tok, dim = y_ref.shape
    half, quarter = tok // 2, tok // 4
    n_buf, width = sw1.shape[0], sw1.shape[2]
    n_chunks = sw1_hbm.shape[1] // width

    def shared_loads(c):
        slot = lax.rem(c, n_buf)
        cols = pl.ds(pl.multiple_of(c * width, width), width)
        return [
            pltpu.make_async_copy(sw1_hbm.at[:, cols], sw1.at[slot], sw_sem.at[slot, 0]),
            pltpu.make_async_copy(sw3_hbm.at[:, cols], sw3.at[slot], sw_sem.at[slot, 1]),
            pltpu.make_async_copy(sw2_hbm.at[cols, :], sw2.at[slot], sw_sem.at[slot, 2]),
        ]

    def first_loads(c, _):
        for load in shared_loads(c):
            load.start()
        return 0

    lax.fori_loop(0, n_buf, first_loads, 0)

    meta_ref[0:top_k, :] = ids_ref[...]
    meta_ref[8 : 8 + top_k, :] = prio_ref[...]

    def norm(i, _):
        rows = pl.ds(pl.multiple_of(i * 16, 16), 16)
        y = y_ref[rows, :].astype(F32)
        inv_rms = lax.rsqrt(jnp.mean(y * y, axis=1, keepdims=True) + NORM_EPS)
        b_ref[rows, :] = (y * inv_rms * gain_ref[...]).astype(BF16)
        return 0

    lax.fori_loop(0, tok // 16, norm, 0)

    barrier = pltpu.get_barrier_semaphore()

    def greet(o, _):
        pl.semaphore_signal(barrier, inc=1, device_id={"ep": lax.rem(me + o, ep)}, device_id_type=MESH)
        return 0

    lax.fori_loop(1, ep, greet, 0)
    pl.semaphore_wait(barrier, ep - 1)

    own = pltpu.make_async_copy(b_ref, yall.at[me], own_sem)
    own.start()

    def meta_copy(o, src):
        return pltpu.make_async_remote_copy(
            src_ref=meta_ref, dst_ref=meta_all.at[src], send_sem=m_send.at[o], recv_sem=m_recv.at[o],
            device_id={"ep": lax.rem(me + o, ep)}, device_id_type=MESH,
        )

    def send_meta(o, _):
        meta_copy(o, me).start()
        return 0

    lax.fori_loop(1, ep, send_meta, 0)

    def piece(fam, g, k, sent):
        j = g - 1
        hop = {0: 1, 1: -1, 2: 1, 3: -1}[k]
        dist = {0: 0 if sent else -1, 1: 0 if sent else 1, 2: -1 if sent else 2, 3: 1 if sent else 2}[k]
        du, dv = (dist, 0) if g == 0 else (j, dist)
        start = fam * half + (quarter if k == 3 else 0)
        size = half if k < 2 else quarter
        return du % side, dv % side, start, size, hop

    def link_copy(fam, g, k, sent):
        du, dv, start, size, hop = piece(fam, g, k, sent)
        block = pc.at(fam, du, dv)
        rows = yall.at[block, pl.ds(start, size), :]
        source = b_ref.at[pl.ds(start, size), :] if sent and (du, dv) == (0, 0) else rows
        target = pc.at(fam, hop, 0) if g == 0 else pc.at(fam, 0, hop)
        n = (fam * (side + 1) + g) * 4 + k
        return pltpu.make_async_remote_copy(
            src_ref=source, dst_ref=rows, send_sem=s_send.at[n], recv_sem=s_recv.at[n], device_id={"ep": target}, device_id_type=MESH
        )

    def pass_on(fam, g, k, mine):
        du, dv, start, size, _ = piece(fam, g, k, False)
        block = pc.at(fam, du, dv, pc.core if mine else 1 - pc.core)
        rows = yall.at[block, pl.ds(start, size), :]
        n = (fam * (side + 1) + g) * 4 + k
        return pltpu.make_async_remote_copy(
            src_ref=rows, dst_ref=rows, send_sem=p_send.at[n], recv_sem=p_recv.at[n], device_id={"ep": pc.partner}, device_id_type=MESH
        )

    def own_to_partner(block):
        return pltpu.make_async_remote_copy(
            src_ref=b_ref, dst_ref=yall.at[block], send_sem=o_send, recv_sem=o_recv, device_id={"ep": pc.partner}, device_id_type=MESH
        )

    for fam in range(2):
        for k in range(2):
            link_copy(fam, 0, k, True).start()
    own_to_partner(me).start()
    for fam in range(2):
        for k in range(2):
            link_copy(fam, 1, k, True).start()

    def wait_meta(o, _):
        meta_copy(o, lax.rem(me - o + ep, ep)).wait_recv()
        return 0

    def gates():
        logits = lax.dot_general(router_ref[...], b_ref[...], (((1,), (1,)), ((), ())), preferred_element_type=F32)
        probs = jnp.exp(logits - jnp.max(logits, axis=0, keepdims=True))
        gate_ref[...] = ROUTE_SCALE * (probs / jnp.sum(probs, axis=0, keepdims=True))

    def shared(c, _):
        slot = lax.rem(c, n_buf)
        for load in shared_loads(c):
            load.wait()
        up_a = jnp.dot(b_ref[...], sw1[slot], preferred_element_type=F32)
        up_b = jnp.dot(b_ref[...], sw3[slot], preferred_element_type=F32)
        act = (up_a * jax.nn.sigmoid(up_a) * up_b).astype(BF16)
        base_ref[...] += jnp.dot(act, sw2[slot], preferred_element_type=F32)

        @pl.when(c + n_buf < n_chunks)
        def _():
            for load in shared_loads(c + n_buf):
                load.start()

        return 0

    base_ref[...] = jnp.zeros(base_ref.shape, F32)
    shared_done = [0]

    def fill_in(n):
        end = min(shared_done[0] + n, n_chunks)
        if end > shared_done[0]:
            lax.fori_loop(shared_done[0], end, shared, 0)
        shared_done[0] = end

    meta_all[me] = meta_ref[...]
    gates()
    lax.fori_loop(1, ep, wait_meta, 0)
    route(pc, ep, top_k, n_local, ep // 2, meta_all, ids, prs, pr, thr, cnt, kch, pos, ka, kb, info_ref, q_ref)

    slots = x_ref.shape[0]
    n_cols = 512
    lane = lax.broadcasted_iota(jnp.int32, (1, tok), 1)

    def pick(halves, first=False):
        depth = len(halves) * tok
        where_to = [[jnp.where(lane < half, pos[l, pl.ds(lo, 1), :], pos[l, pl.ds(hi, 1), :]) for l in range(n_local)] for lo, hi in halves]

        def build(i, _):
            rows = pl.ds(pl.multiple_of(i * TILE, TILE), TILE)
            slot = lax.broadcasted_iota(jnp.int32, (TILE, tok), 0) + i * TILE
            for n, places in enumerate(where_to):
                hit = slot == places[0]
                for place in places[1:]:
                    hit = hit | (slot == place)
                sel[rows, n * tok : (n + 1) * tok] = jnp.where(hit, 1.0, 0.0).astype(BF16)
            return 0

        lax.fori_loop(0, slots // TILE, build, 0)

        def one(n, _):
            cols = pl.ds(pl.multiple_of(n * n_cols, n_cols), n_cols)
            pieces = []
            for lo, hi in halves:
                pieces += [yall[lo, :half, cols], yall[hi, half:, cols]]
            picked = jnp.dot(sel[:, :depth], jnp.concatenate(pieces, axis=0), preferred_element_type=F32).astype(BF16)
            x_ref[:, cols] = picked if first else x_ref[:, cols] + picked
            return 0

        lax.fori_loop(0, dim // n_cols, one, 0)

    def two(ks):
        return [(f, k) for f in range(2) for k in ks]

    steps = [(0, (0, 1)), (1, (0, 1)), (0, (2, 3)), (side, (0, 1)), (2, (0, 1)), (1, (2, 3)), (3, (0, 1))]
    steps += [(g, (2, 3)) for g in (side, 2, 3)]

    def receive(g, ks):
        for f, k in two(ks):
            link_copy(f, g, k, False).wait_recv()
            if k < 2:
                link_copy(f, g, k + 2, True).start()
        if g == 0:
            for j in (side - 1, 1) if ks == (0, 1) else (2,):
                for f, k in two((0, 1)):
                    link_copy(f, 1 + j, k, True).start()
        for f, k in two(ks):
            pass_on(f, g, k, True).start()

    def take(g, ks):
        for f, k in two(ks):
            pass_on(f, g, k, False).wait_recv()
        halves = []
        for k in ks if ks == (0, 1) else (2,):
            for core in (pc.core, 1 - pc.core):
                halves.append(tuple(pc.at(f, *piece(f, g, k, False)[:2], core) for f in range(2)))
        pick(halves)

    own.wait()
    own_to_partner(pc.partner).wait_recv()
    pick([(me, me), (pc.partner, pc.partner)], first=True)
    for i, step in enumerate(steps):
        receive(*step)
        if i > 0:
            take(*steps[i - 1])
        if i in (1, 3, 4, 6):
            fill_in(3)
    take(*steps[-1])
    x_out = pltpu.make_async_copy(x_ref, x_hbm, x_sem)
    x_out.start()
    base_ref[...] = y_ref[...].astype(F32) + base_ref[...].astype(BF16).astype(F32)

    def sent_meta(o, _):
        meta_copy(o, me).wait_send()
        return 0

    lax.fori_loop(1, ep, sent_meta, 0)
    own_to_partner(me).wait_send()
    for g, ks in steps:
        for f, k in two(ks):
            link_copy(f, g, k, True).wait_send()
            pass_on(f, g, k, True).wait_send()
    x_out.wait()


def dispatch(ep, n_local, resid_in, expert_ids, priority, norm_gain, router_w, shared_w1, shared_w3, shared_w2):
    tok, dim = resid_in.shape
    top_k = expert_ids.shape[1]
    side = math.isqrt(ep // 2)
    n_exp = ep * n_local
    slots = tok * top_k + (n_local - 1) * TILE
    n_piece = 2 * (side + 1) * 4
    n_buf, width = 3, 256
    vmem = pl.BlockSpec(memory_space=pltpu.VMEM)
    hbm = pl.BlockSpec(memory_space=pl.ANY)
    dma = pltpu.SemaphoreType.DMA
    return pl.pallas_call(
        functools.partial(dispatch_kernel, ep, top_k, n_local),
        out_shape=(
            jax.ShapeDtypeStruct((slots, dim), BF16),
            jax.ShapeDtypeStruct((8, 128), jnp.int32),
            jax.ShapeDtypeStruct((n_exp, tok), jnp.int32),
            jax.ShapeDtypeStruct((n_exp, tok), F32),
            jax.ShapeDtypeStruct((tok, dim), F32),
        ),
        in_specs=[vmem] * 5 + [hbm] * 3,
        out_specs=(hbm, vmem, vmem, vmem, vmem),
        scratch_shapes=[
            pltpu.VMEM((slots, dim), BF16),
            pltpu.VMEM((tok, dim), BF16),
            pltpu.VMEM((16, tok), jnp.int32),
            pltpu.VMEM((ep, tok, dim), BF16),
            pltpu.VMEM((ep, 16, tok), jnp.int32),
            pltpu.VMEM((top_k, ep, tok), jnp.int32),
            pltpu.VMEM((top_k, ep, tok), jnp.int32),
            pltpu.VMEM((n_exp, ep, tok), jnp.int32),
            pltpu.VMEM((ep, tok), jnp.int32),
            pltpu.VMEM((ep, tok), F32),
            pltpu.VMEM((ep * ep, tok), F32),
            pltpu.VMEM((n_local, ep, tok), jnp.int32),
            pltpu.VMEM((n_exp, tok), F32),
            pltpu.VMEM((n_exp, tok), F32),
            pltpu.VMEM((slots, 4 * tok), BF16),
            pltpu.VMEM((n_buf, dim, width), BF16),
            pltpu.VMEM((n_buf, dim, width), BF16),
            pltpu.VMEM((n_buf, width, dim), BF16),
            dma(()), dma(()), dma((n_buf, 3)),
            dma((ep,)), dma((ep,)), dma((n_piece,)), dma((n_piece,)), dma((n_piece,)), dma((n_piece,)), dma(()), dma(()),
        ],
        compiler_params=pltpu.CompilerParams(collective_id=0, has_side_effects=True, vmem_limit_bytes=VMEM_LIMIT),
        name="dispatch",
    )(
        resid_in, expert_ids.T, priority.T, norm_gain.reshape(1, dim), router_w.T, shared_w1, shared_w3, shared_w2,
    )


def expert_kernel(ep, sc, x_hbm, w1_hbm, w3_hbm, w2_hbm, e_hbm, a_ref, b_ref, x_ref, e_ref, act, w1, w3, w2, x_sem, e_sem, sems):
    n_local, dim, ff = w1.shape
    slots = x_ref.shape[0]
    parts = [(c, min(512, ff - c)) for c in range(0, ff, 512)]
    x_in = pltpu.make_async_copy(x_hbm, x_ref, x_sem)

    def loads(l, n):
        if n == len(parts):
            return [pltpu.make_async_copy(w2_hbm.at[l], w2.at[l], sems.at[l, 2 * n])]
        cols = pl.ds(*parts[n])
        return [
            pltpu.make_async_copy(w1_hbm.at[l, :, cols], w1.at[l, :, cols], sems.at[l, 2 * n]),
            pltpu.make_async_copy(w3_hbm.at[l, :, cols], w3.at[l, :, cols], sems.at[l, 2 * n + 1]),
        ]

    def request(l, n):
        l, n = (l, n) if n <= len(parts) else (l + 1, n - len(parts) - 1)

        @pl.when(l < n_local)
        def _():
            for load in loads(l, n):
                load.start()

    def arrive(l, n):
        for load in loads(l, n):
            load.wait()
        request(l, n + 2)

    x_in.start()
    request(0, 0)
    request(0, 1)

    def over_tiles(first, count, body):
        def once(i, _):
            body(pl.ds(pl.multiple_of((first + i) * TILE, TILE), TILE))
            return 0

        lax.fori_loop(0, count, once, 0)

    x_in.wait()

    def one_expert(l, done):
        count = (sc[2 * l + 1, ep - 1] - sc[2 * l + 1, 0] + sc[2 * l, ep - 1] + TILE - 1) // TILE
        for n, (c, size) in enumerate(parts):
            arrive(l, n)

            def up(rows, c=c, size=size):
                x = x_ref[rows, :]
                up_a = jnp.dot(x, w1[l, :, c : c + size], preferred_element_type=F32)
                up_b = jnp.dot(x, w3[l, :, c : c + size], preferred_element_type=F32)
                act[rows, c : c + size] = (up_a * jax.nn.sigmoid(up_a) * up_b).astype(BF16)

            over_tiles(done, count, up)
        arrive(l, len(parts))

        def down(rows):
            e_ref[rows, :] = jnp.dot(act[rows, :], w2[l], preferred_element_type=F32).astype(BF16)

        over_tiles(done, count, down)
        return done + count

    done = lax.fori_loop(0, n_local, one_expert, 0)

    def clear(i, _):
        rows = pl.ds(pl.multiple_of(i * TILE, TILE), TILE)
        e_ref[rows, :] = jnp.zeros((TILE, dim), BF16)
        return 0

    lax.fori_loop(done, slots // TILE, clear, 0)
    e_out = pltpu.make_async_copy(e_ref, e_hbm, e_sem)
    e_out.start()
    fill_buckets(ep, sc, 0, e_ref, a_ref, b_ref, n_local)
    e_out.wait()


def bucket_shape(ep, dim):
    side = math.isqrt(ep // 2)
    return jax.ShapeDtypeStruct((side, 2, side, CAP, dim // 4), BF16)


def experts(ep, info, x, expert_w1, expert_w3, expert_w2):
    vmem = pl.BlockSpec(memory_space=pltpu.VMEM)
    hbm = pl.BlockSpec(memory_space=pl.ANY)
    n_local, dim, ff = expert_w1.shape
    bucket = bucket_shape(ep, dim)
    return pl.pallas_call(
        functools.partial(expert_kernel, ep),
        out_shape=(jax.ShapeDtypeStruct(x.shape, BF16), bucket, bucket),
        in_specs=[pl.BlockSpec(memory_space=pltpu.SMEM), hbm, hbm, hbm, hbm],
        out_specs=(hbm, vmem, vmem),
        scratch_shapes=[
            pltpu.VMEM(x.shape, BF16),
            pltpu.VMEM(x.shape, BF16),
            pltpu.VMEM((x.shape[0], ff), BF16),
            pltpu.VMEM((n_local, dim, ff), BF16),
            pltpu.VMEM((n_local, dim, ff), BF16),
            pltpu.VMEM((n_local, ff, dim), BF16),
            pltpu.SemaphoreType.DMA(()),
            pltpu.SemaphoreType.DMA(()),
            pltpu.SemaphoreType.DMA((n_local, 2 * (-(-ff // 512)) + 1)),
        ],
        compiler_params=pltpu.CompilerParams(vmem_limit_bytes=VMEM_LIMIT),
        name="experts",
    )(info, x, expert_w1, expert_w3, expert_w2)


def fill_kernel(ep, n_local, sc, rnd, e_ref, a_ref, b_ref):
    fill_buckets(ep, sc, rnd[0], e_ref, a_ref, b_ref, n_local)


def fill_buckets(ep, sc, rnd, e_ref, a_ref, b_ref, n_local):
    pc = Place(ep)
    side = pc.side
    slots, dim = e_ref.shape
    width = dim // 4
    window = (CAP + 15 + 15) // 16 * 16
    skip = rnd * CAP

    def one(n, _):
        dx, dy = lax.rem(n, side), n // side
        chip = lax.rem(pc.py + dy, side) * side + lax.rem(pc.px + dx, side)
        row = lax.broadcasted_iota(jnp.int32, (CAP, window), 0)
        col = lax.broadcasted_iota(jnp.int32, (CAP, window), 1)
        picks, sources = [], []
        lead = -skip
        for l in range(n_local):
            start, count = sc[2 * l + 1, 2 * chip], sc[2 * l, 2 * chip] + sc[2 * l, 2 * chip + 1]
            used = jnp.minimum(jnp.maximum(-lead, 0), count)
            origin = jnp.minimum((start + used) // 16 * 16, slots - window)
            origin = pl.multiple_of(origin, 16)
            slot = row - lead + start
            hit = (slot == col + origin) & (row >= lead) & (row < lead + count)
            picks.append(jnp.where(hit, 1.0, 0.0).astype(BF16))
            sources.append(e_ref[pl.ds(origin, window), :])
            lead = lead + count
        out = jnp.dot(picks[0], sources[0], preferred_element_type=F32)
        for l in range(1, n_local):
            out = out + jnp.dot(picks[l], sources[l], preferred_element_type=F32)
        out = out.astype(BF16)
        for c in range(2):
            a_ref[dx, c, dy] = out[:, c * width : (c + 1) * width]
            b_ref[dy, c, dx] = out[:, (2 + c) * width : (3 + c) * width]
        return 0

    lax.fori_loop(0, side * side, one, 0, unroll=4)


def fill(ep, n_local, info, rnd, e):
    vmem = pl.BlockSpec(memory_space=pltpu.VMEM)
    smem = pl.BlockSpec(memory_space=pltpu.SMEM)
    bucket = bucket_shape(ep, e.shape[1])
    return pl.pallas_call(
        functools.partial(fill_kernel, ep, n_local),
        out_shape=(bucket, bucket),
        in_specs=[smem, smem, vmem],
        out_specs=(vmem, vmem),
        compiler_params=pltpu.CompilerParams(vmem_limit_bytes=VMEM_LIMIT),
        name="fill",
    )(info, rnd, e)


def combine_kernel(
    ep, n_local, bka, bkb, q_ref, p_ref, acc_ref, out_ref, st, rl, fin, ry, pf, g_ref, s_send, s_recv, p_send, p_recv
):
    pc = Place(ep)
    side = pc.side
    tok = q_ref.shape[1]
    width = bka.shape[-1]
    bk = (bka, bkb)

    barrier = pltpu.get_barrier_semaphore()
    friends = [pc.dev(1, 0), pc.dev(-1, 0), pc.dev(0, 1), pc.dev(0, -1), pc.partner]
    for friend in friends:
        pl.semaphore_signal(barrier, inc=1, device_id={"ep": friend}, device_id_type=MESH)
    pl.semaphore_wait(barrier, len(friends))

    def held(fam, j):
        return bk[fam].at[0] if j == 0 else st.at[fam, j]

    def link_copy(fam, g, k):
        hop = 1 if k % 2 == 0 else -1
        c = k % 2
        if g == 0:
            target = pc.at(fam, hop, 0)
            if k < 2:
                src, dst = bk[fam].at[hop % side], st.at[fam, hop % side]
            elif k < 4:
                src, dst = bk[fam].at[2, c], rl.at[fam, c]
            else:
                src, dst = rl.at[fam, c], st.at[fam, 2, c]
        else:
            j = g - 1
            target = pc.at(fam, 0, hop)
            if k < 2:
                src, dst = held(fam, j).at[:, hop % side], fin.at[fam, j, hop % side]
            elif k < 4:
                src, dst = held(fam, j).at[c, 2], ry.at[fam, j, c]
            else:
                src, dst = ry.at[fam, j, c], fin.at[fam, j, 2, c]
        n = (fam * (side + 1) + g) * 6 + k
        return pltpu.make_async_remote_copy(
            src_ref=src, dst_ref=dst, send_sem=s_send.at[n], recv_sem=s_recv.at[n], device_id={"ep": target}, device_id_type=MESH
        )

    def arrived(fam, j, v):
        return held(fam, j).at[:, 0] if v == 0 else fin.at[fam, j, v]

    def pass_on(fam, j, v):
        n = (fam * side + j) * side + v
        return pltpu.make_async_remote_copy(
            src_ref=arrived(fam, j, v), dst_ref=pf.at[fam, j, v], send_sem=p_send.at[n], recv_sem=p_recv.at[n],
            device_id={"ep": pc.partner}, device_id_type=MESH,
        )

    for k in (2, 3, 0, 1):
        for fam in range(2):
            link_copy(fam, 0, k).start()
    for k in (2, 3, 0, 1):
        for fam in range(2):
            link_copy(fam, 1, k).start()
    for fam in range(2):
        pass_on(fam, 0, 0).start()

    row = lax.broadcasted_iota(jnp.int32, (g_ref.shape[3], tok), 0)

    def weights(d, _):
        w = jnp.zeros(row.shape, F32)
        for l in range(n_local):
            e = d * n_local + l
            w = w + jnp.where(row == q_ref[pl.ds(e, 1), :], p_ref[pl.ds(e, 1), :], 0.0)
        w = w.T
        for n in range(3):
            term = w.astype(BF16)
            g_ref[d, n] = term
            w = w - term.astype(F32)
        return 0

    lax.fori_loop(0, ep, weights, 0)
    out_ref[...] = acc_ref[...]

    def add(fam, j, v):
        devs = [pc.at(fam, -j, -v), pc.at(fam, -j, -v, 1 - pc.core)]

        def one(c, _):
            cols = pl.ds(pl.multiple_of((2 * fam + c) * width, width), width)
            total = out_ref[:, cols]
            for d, rows in zip(devs, (arrived(fam, j, v), pf.at[fam, j, v])):
                data = rows[c]
                for n in range(3):
                    total = total + jnp.dot(g_ref[d, n][:, :CAP], data, preferred_element_type=F32)
            out_ref[:, cols] = total
            return 0

        lax.fori_loop(0, 2, one, 0)

    ready = []

    def here(fam, j, v):
        pass_on(fam, j, v).start()
        ready.append((fam, j, v))

    def drain(keep):
        while len(ready) > keep:
            fam, j, v = ready.pop(0)
            pass_on(fam, j, v).wait_recv()
            add(fam, j, v)

    def got(fam, g, k):
        link_copy(fam, g, k).wait_recv()

    ready += [(0, 0, 0), (1, 0, 0)]
    for k in (2, 3):
        for fam in range(2):
            got(fam, 0, k)
            link_copy(fam, 0, k + 2).start()
    drain(0)
    for k in (0, 1):
        for fam in range(2):
            got(fam, 0, k)
            j = 1 if k == 0 else side - 1
            for kk in (2, 3, 0, 1):
                link_copy(fam, 1 + j, kk).start()
            here(fam, j, 0)
    for k in (2, 3):
        for fam in range(2):
            got(fam, 1, k)
            link_copy(fam, 1, k + 2).start()
    for fam in range(2):
        got(fam, 0, 4)
        got(fam, 0, 5)
        for kk in (2, 3, 0, 1):
            link_copy(fam, 3, kk).start()
        here(fam, 2, 0)
    drain(2)
    for j in (0, 1, side - 1, 2):
        if j > 0:
            for k in (2, 3):
                for fam in range(2):
                    got(fam, 1 + j, k)
                    link_copy(fam, 1 + j, k + 2).start()
        for k in (0, 1):
            for fam in range(2):
                got(fam, 1 + j, k)
                here(fam, j, 1 if k == 0 else side - 1)
        drain(2)
    for j in (0, 1, side - 1, 2):
        for fam in range(2):
            got(fam, 1 + j, 4)
            got(fam, 1 + j, 5)
            here(fam, j, 2)
        drain(2)
    drain(0)
    for fam in range(2):
        for g in range(side + 1):
            for k in range(6):
                link_copy(fam, g, k).wait_send()
        for j in range(side):
            for v in range(side):
                pass_on(fam, j, v).wait_send()


def combine(ep, n_local, bka, bkb, q, weights, acc):
    side = math.isqrt(ep // 2)
    cap, width = bka.shape[-2:]
    tok = q.shape[1]
    vmem = pl.BlockSpec(memory_space=pltpu.VMEM)
    dma = pltpu.SemaphoreType.DMA
    n_link, n_pass = 2 * (side + 1) * 6, 2 * side * side
    return pl.pallas_call(
        functools.partial(combine_kernel, ep, n_local),
        out_shape=jax.ShapeDtypeStruct(acc.shape, F32),
        in_specs=[vmem] * 5,
        out_specs=vmem,
        scratch_shapes=[
            pltpu.VMEM((2, side, 2, side, cap, width), BF16),
            pltpu.VMEM((2, 2, side, cap, width), BF16),
            pltpu.VMEM((2, side, side, 2, cap, width), BF16),
            pltpu.VMEM((2, side, 2, cap, width), BF16),
            pltpu.VMEM((2, side, side, 2, cap, width), BF16),
            pltpu.VMEM((ep, 3, tok, tok), BF16),
            dma((n_link,)), dma((n_link,)), dma((n_pass,)), dma((n_pass,)),
        ],
        compiler_params=pltpu.CompilerParams(collective_id=1, has_side_effects=True, vmem_limit_bytes=VMEM_LIMIT),
        name="combine",
    )(bka, bkb, q, weights, acc)


def solution(mesh):
    ep = mesh.shape["ep"]
    tok_spec = P(("dp", "ep"))
    expert_spec = P("ep")

    def device_fn(resid_in, expert_ids, priority, norm_gain, router_w, shared_w1, shared_w3, shared_w2, expert_w1, expert_w3, expert_w2):
        n_local = expert_w1.shape[0]
        x, info, q, gates, base = dispatch(
            ep, n_local, resid_in, expert_ids, priority, norm_gain, router_w, shared_w1, shared_w3, shared_w2
        )
        e, bka, bkb = experts(ep, info, x, expert_w1, expert_w3, expert_w2)
        first = combine(ep, n_local, bka, bkb, q, gates, base)
        rounds = lax.div(info[2 * n_local, 0] + (CAP - 1), CAP)

        def one_round(carry):
            rnd, acc = carry
            more_a, more_b = fill(ep, n_local, info, rnd[None], e)
            return rnd + 1, combine(ep, n_local, more_a, more_b, q - rnd * CAP, gates, acc)

        total = lax.while_loop(lambda carry: carry[0] < rounds, one_round, (jnp.int32(1), first))[1]
        return total.astype(BF16)

    return jax.shard_map(
        device_fn, mesh=mesh,
        in_specs=(tok_spec, tok_spec, tok_spec, P(), P(), P(), P(), P(), expert_spec, expert_spec, expert_spec),
        out_specs=tok_spec, check_vma=False,
    )
```

```python
import functools
import math

import jax
import jax.numpy as jnp
from jax import lax
from jax.experimental import pallas as pl
from jax.experimental.pallas import tpu as pltpu
from jax.sharding import PartitionSpec as P

NORM_EPS = 1e-6
ROUTE_SCALE = 16.0
MESH = pl.DeviceIdType.MESH
F32 = jnp.float32
BF16 = jnp.bfloat16
PAIR = (0, 1)
SPLIT = (2, 3)
SENDS = SPLIT + PAIR
LANES = (((1,), (1,)), ((), ()))
FAR = 1 << 20
TILE = 128
PARTS = ((0, 512), (512, 1024))
AHEAD = 2
CAP = 72
VMEM_LIMIT = 64000 * 1024


class Place:
    def __init__(self, ep):
        self.side = math.isqrt(ep // 2)
        self.me = lax.axis_index("ep")
        self.core = lax.rem(self.me, 2)
        self.chip = self.me // 2
        self.px = lax.rem(self.chip, self.side)
        self.py = self.chip // self.side
        self.partner = self.me + 1 - 2 * self.core

    def dev(self, dx, dy, core=None):
        x = lax.rem(self.px + dx % self.side, self.side)
        y = lax.rem(self.py + dy % self.side, self.side)
        return (y * self.side + x) * 2 + (self.core if core is None else core)

    def at(self, fam, du, dv, core=None):
        return self.dev(du, dv, core) if fam == 0 else self.dev(dv, du, core)


def loop(n, body, start=0, unroll=1):
    def step(i, carry):
        body(i)
        return carry

    lax.fori_loop(start, n, step, 0, unroll=unroll)


def iota(shape, axis):
    return lax.broadcasted_iota(jnp.int32, shape, axis)


def tri(n, m, rows_first):
    i = iota((n, m), 0)
    j = iota((n, m), 1)
    return jnp.where(i < j if rows_first else j < i, 1.0, 0.0).astype(BF16)


def mm(a, b):
    return jnp.dot(a.astype(BF16), b.astype(BF16), preferred_element_type=F32)


def mm_t(a, b):
    return lax.dot_general(a.astype(BF16), b.astype(BF16), LANES, preferred_element_type=F32)


def route(pc, ep, top_k, n_local, n_chips, meta_all, ids, prs, pr, thr, cnt, kch, pos, ka, kb, info_ref, q_ref):
    n_exp = ep * n_local
    tok = ids.shape[2]
    capacity = tok * top_k
    n_bits = (ep * capacity).bit_length()

    def unpack(s):
        for k in range(top_k):
            ids[k, pl.ds(s, 1), :] = meta_all[s, k : k + 1, :]
            prs[k, pl.ds(s, 1), :] = meta_all[s, top_k + k : top_k + k + 1, :]

    loop(ep, unpack)

    def per_expert(e):
        best = jnp.full((ep, tok), FAR, jnp.int32)
        for k in range(top_k):
            best = jnp.minimum(best, jnp.where(ids[k] == e, prs[k], FAR))
        pr[e] = best

    loop(n_exp, per_expert)

    thr[...] = jnp.zeros(thr.shape, jnp.int32)

    def bit_step(i, step):
        for d in range(ep):
            cand = thr[d : d + 1, :] + step
            hits = jnp.zeros((ep, tok), F32)
            for l in range(n_local):
                hits = hits + jnp.where(pr[d * n_local + l] < cand, 1.0, 0.0)
            cnt[d : d + 1, :] = jnp.sum(hits, axis=0, keepdims=True)
        total = jnp.sum(cnt[...], axis=1, keepdims=True)
        thr[...] = thr[...] + jnp.where(total <= capacity, step, 0)
        return step // 2

    lax.fori_loop(0, n_bits, bit_step, jnp.int32(1 << (n_bits - 1)))

    def chip_counts(d):
        kept = jnp.zeros((ep, tok), F32)
        for l in range(n_local):
            kept = kept + jnp.where(pr[d * n_local + l] < thr[pl.ds(d, 1), :], 1.0, 0.0)
        kch[pl.ds(pl.multiple_of(d * ep, ep), ep), :] = kept

    loop(ep, chip_counts)
    pairs = kch[pl.ds(0, ep * n_chips, stride=2), :] + kch[pl.ds(1, ep * n_chips, stride=2), :]
    worst = jnp.max(jnp.sum(pairs, axis=1, keepdims=True), axis=0, keepdims=True)
    info_ref[...] = jnp.broadcast_to(worst, info_ref.shape).astype(jnp.int32)
    upper = tri(tok, tok, True)
    ones = jnp.ones((tok, tok), BF16)
    lower = tri(ep, ep, False)
    my_thr = thr[pl.ds(pc.me, 1), :]
    base = jnp.zeros((1, tok), F32)
    for l in range(n_local):
        kept = pr[pc.me * n_local + l] < my_thr
        kept_f = jnp.where(kept, 1.0, 0.0)
        in_row = mm(kept_f, upper)
        row_total = mm(kept_f, ones)
        row_start = mm(lower, row_total)
        pos[l] = jnp.where(kept, (in_row + row_start + base), -1.0).astype(jnp.int32)
        totals = mm_t(jnp.ones((8, tok), F32), kept_f)
        starts = mm(totals, tri(ep, ep, True)) + base[:, :ep]
        info_ref[2 * l : 2 * l + 1, :ep] = totals[:1].astype(jnp.int32)
        info_ref[2 * l + 1 : 2 * l + 2, :ep] = starts[:1].astype(jnp.int32)
        group = jnp.sum(row_total, axis=0, keepdims=True)
        base = base + jnp.floor((group + (TILE - 1)) * (1.0 / TILE)) * TILE

    def chip_rows(e):
        limit = thr[pl.ds(e // n_local, 1), :]
        first = pr[e, pl.ds(pc.chip * 2, 1), :]
        second = pr[e, pl.ds(pc.chip * 2 + 1, 1), :]
        ka[pl.ds(e, 1), :] = jnp.where(first < limit, 1.0, 0.0)
        kb[pl.ds(e, 1), :] = jnp.where(second < limit, 1.0, 0.0)

    loop(n_exp, chip_rows)
    k_a, k_b = ka[...], kb[...]
    tot_a = mm(k_a, ones)
    both = tot_a + mm(k_b, ones)
    i = iota((n_exp, n_exp), 0)
    j = iota((n_exp, n_exp), 1)
    earlier = jnp.where((j < i) & (j // n_local == i // n_local), 1.0, 0.0)
    before = mm(earlier, both)
    q_a = jnp.where(k_a > 0, mm(k_a, upper) + before, -1.0)
    q_b = jnp.where(k_b > 0, mm(k_b, upper) + tot_a + before, -1.0)
    second_core = iota(q_ref.shape, 0) * 0 + pc.core
    q_ref[...] = jnp.where(second_core == 0, q_a, q_b).astype(jnp.int32)


def dispatch_kernel(
    ep, top_k, n_local, y_ref, ids_ref, prio_ref, gain_ref, router_ref, sw1_hbm, sw3_hbm, sw2_hbm,
    x_hbm, info_ref, q_ref, gate_ref, base_ref,
    x_ref, b_ref, meta_ref, yall, meta_all, ids, prs, pr, thr, cnt, kch, pos, ka, kb, sel, sw1, sw3, sw2,
    own_sem, x_sem, sw_sem, m_send, m_recv, s_send, s_recv, p_send, p_recv, o_send, o_recv,
):
    pc = Place(ep)
    side, me = pc.side, pc.me
    tok, dim = y_ref.shape
    half, quarter, n_chips = tok // 2, tok // 4, ep // 2
    n_buf, width = sw1.shape[0], sw1.shape[2]
    n_chunks = sw1_hbm.shape[1] // width

    def shared_loads(c):
        slot = lax.rem(c, n_buf)
        cols = pl.ds(pl.multiple_of(c * width, width), width)
        return [
            pltpu.make_async_copy(sw1_hbm.at[:, cols], sw1.at[slot], sw_sem.at[slot, 0]),
            pltpu.make_async_copy(sw3_hbm.at[:, cols], sw3.at[slot], sw_sem.at[slot, 1]),
            pltpu.make_async_copy(sw2_hbm.at[cols, :], sw2.at[slot], sw_sem.at[slot, 2]),
        ]

    def first_loads(c):
        for load in shared_loads(c):
            load.start()

    loop(n_buf, first_loads)

    meta_ref[0:top_k, :] = ids_ref[...]
    meta_ref[top_k:, :] = prio_ref[...]

    def norm(i):
        rows = pl.ds(pl.multiple_of(i * 16, 16), 16)
        y = y_ref[rows, :].astype(F32)
        inv_rms = lax.rsqrt(jnp.mean(y * y, axis=1, keepdims=True) + NORM_EPS)
        b_ref[rows, :] = (y * inv_rms * gain_ref[...]).astype(BF16)

    loop(tok // 16, norm)

    barrier = pltpu.get_barrier_semaphore()

    def greet(o):
        pl.semaphore_signal(barrier, inc=1, device_id={"ep": lax.rem(me + 2 * o, ep)}, device_id_type=MESH)

    loop(n_chips, greet, 1)
    pl.semaphore_signal(barrier, inc=1, device_id={"ep": pc.partner}, device_id_type=MESH)
    pl.semaphore_wait(barrier, n_chips)

    own = pltpu.make_async_copy(b_ref, yall.at[me], own_sem)
    own.start()

    def meta_copy(o, src):
        return pltpu.make_async_remote_copy(
            src_ref=meta_ref, dst_ref=meta_all.at[src], send_sem=m_send.at[o], recv_sem=m_recv.at[o],
            device_id={"ep": lax.rem(me + 2 * o, ep)}, device_id_type=MESH,
        )

    def meta_pass(o, origin, src=None):
        block = lax.rem(origin - 2 * o + ep, ep)
        return pltpu.make_async_remote_copy(
            src_ref=meta_all.at[block] if src is None else src, dst_ref=meta_all.at[block],
            send_sem=m_send.at[n_chips + o], recv_sem=m_recv.at[n_chips + o], device_id={"ep": pc.partner}, device_id_type=MESH,
        )

    def send_meta(o):
        meta_copy(o, me).start()

    loop(n_chips, send_meta, 1)
    meta_pass(0, me, meta_ref).start()

    def piece(fam, g, k, sent):
        j = g - 1
        hop = -1 if k % 2 else 1
        dist = (0 if sent else -hop) if k in PAIR else (-hop if sent else 2)
        du, dv = (dist, 0) if g == 0 else (j, dist)
        start = fam * half + (quarter if k == 3 else 0)
        size = half if k < 2 else quarter
        return du % side, dv % side, start, size, hop

    def link_copy(fam, g, k, sent):
        du, dv, start, size, hop = piece(fam, g, k, sent)
        block = pc.at(fam, du, dv)
        rows = yall.at[block, pl.ds(start, size), :]
        source = b_ref.at[pl.ds(start, size), :] if sent and (du, dv) == (0, 0) else rows
        target = pc.at(fam, hop, 0) if g == 0 else pc.at(fam, 0, hop)
        n = (fam * (side + 1) + g) * 4 + k
        return pltpu.make_async_remote_copy(
            src_ref=source, dst_ref=rows, send_sem=s_send.at[n], recv_sem=s_recv.at[n], device_id={"ep": target}, device_id_type=MESH
        )

    def pass_on(fam, g, k, mine):
        du, dv, start, size, _ = piece(fam, g, k, False)
        block = pc.at(fam, du, dv, pc.core if mine else 1 - pc.core)
        rows = yall.at[block, pl.ds(start, size), :]
        n = (fam * (side + 1) + g) * 4 + k
        return pltpu.make_async_remote_copy(
            src_ref=rows, dst_ref=rows, send_sem=p_send.at[n], recv_sem=p_recv.at[n], device_id={"ep": pc.partner}, device_id_type=MESH
        )

    def own_to_partner(block):
        return pltpu.make_async_remote_copy(
            src_ref=b_ref, dst_ref=yall.at[block], send_sem=o_send, recv_sem=o_recv, device_id={"ep": pc.partner}, device_id_type=MESH
        )

    for fam in PAIR:
        for k in PAIR:
            link_copy(fam, 0, k, True).start()
    own_to_partner(me).start()
    for fam in PAIR:
        for k in PAIR:
            link_copy(fam, 1, k, True).start()

    def wait_meta(o):
        meta_copy(o, lax.rem(me - 2 * o + ep, ep)).wait_recv()
        meta_pass(o, me).start()

    def wait_passed(o):
        meta_pass(o, pc.partner).wait_recv()

    def gates():
        logits = lax.dot_general(router_ref[...], b_ref[...], LANES, preferred_element_type=F32)
        probs = jnp.exp(logits - jnp.max(logits, axis=0, keepdims=True))
        gate_ref[...] = ROUTE_SCALE * (probs / jnp.sum(probs, axis=0, keepdims=True))

    def shared(c):
        slot = lax.rem(c, n_buf)
        for load in shared_loads(c):
            load.wait()
        up_a = jnp.dot(b_ref[...], sw1[slot], preferred_element_type=F32)
        up_b = jnp.dot(b_ref[...], sw3[slot], preferred_element_type=F32)
        act = (up_a * jax.nn.sigmoid(up_a) * up_b).astype(BF16)
        base_ref[...] += jnp.dot(act, sw2[slot], preferred_element_type=F32)

        @pl.when(c + n_buf < n_chunks)
        def _():
            for load in shared_loads(c + n_buf):
                load.start()

    base_ref[...] = jnp.zeros(base_ref.shape, F32)
    shared_done = [0]

    def fill_in(n):
        end = min(shared_done[0] + n, n_chunks)
        if end > shared_done[0]:
            loop(end, shared, shared_done[0])
        shared_done[0] = end

    meta_all[me] = meta_ref[...]
    gates()
    loop(n_chips, wait_meta, 1)
    loop(n_chips, wait_passed)
    route(pc, ep, top_k, n_local, n_chips, meta_all, ids, prs, pr, thr, cnt, kch, pos, ka, kb, info_ref, q_ref)

    slots = x_ref.shape[0]
    n_cols = 512
    lane = iota((1, tok), 1)

    def pick(halves, first=False):
        depth = len(halves) * tok
        where_to = [[jnp.where(lane < half, pos[l, pl.ds(lo, 1), :], pos[l, pl.ds(hi, 1), :]) for l in range(n_local)] for lo, hi in halves]

        def build(i):
            rows = pl.ds(pl.multiple_of(i * TILE, TILE), TILE)
            slot = iota((TILE, tok), 0) + i * TILE
            for n, places in enumerate(where_to):
                hit = slot == places[0]
                for place in places[1:]:
                    hit = hit | (slot == place)
                sel[rows, n * tok : (n + 1) * tok] = jnp.where(hit, 1.0, 0.0).astype(BF16)

        loop(slots // TILE, build)

        def one(n):
            cols = pl.ds(pl.multiple_of(n * n_cols, n_cols), n_cols)
            pieces = []
            for lo, hi in halves:
                pieces += [yall[lo, :half, cols], yall[hi, half:, cols]]
            picked = jnp.dot(sel[:, :depth], jnp.concatenate(pieces, axis=0), preferred_element_type=F32).astype(BF16)
            x_ref[:, cols] = picked if first else x_ref[:, cols] + picked

        loop(dim // n_cols, one)

    def two(ks):
        return [(f, k) for f in PAIR for k in ks]

    steps = [(0, PAIR), (1, PAIR), (0, SPLIT), (side, PAIR), (2, PAIR), (1, SPLIT), (3, PAIR)]
    steps += [(g, SPLIT) for g in (side, 2, 3)]

    def receive(g, ks):
        for f, k in two(ks):
            link_copy(f, g, k, False).wait_recv()
            if k < 2:
                link_copy(f, g, k + 2, True).start()
        if g == 0:
            for j in (side - 1, 1) if ks == PAIR else (2,):
                for f, k in two(PAIR):
                    link_copy(f, 1 + j, k, True).start()
        for f, k in two(ks):
            pass_on(f, g, k, True).start()

    def take(g, ks):
        for f, k in two(ks):
            pass_on(f, g, k, False).wait_recv()
        halves = []
        for k in ks if ks == PAIR else (2,):
            for core in (pc.core, 1 - pc.core):
                halves.append(tuple(pc.at(f, *piece(f, g, k, False)[:2], core) for f in PAIR))
        pick(halves)

    own.wait()
    own_to_partner(pc.partner).wait_recv()
    pick([(me, me), (pc.partner, pc.partner)], first=True)
    for i, step in enumerate(steps):
        receive(*step)
        if i > 0:
            take(*steps[i - 1])
        if i in (1, 3, 4, 6):
            fill_in(3)
    take(*steps[-1])
    x_out = pltpu.make_async_copy(x_ref, x_hbm, x_sem)
    x_out.start()
    base_ref[...] = y_ref[...].astype(F32) + base_ref[...].astype(BF16).astype(F32)

    def sent_meta(o):
        meta_copy(o, me).wait_send()
        meta_pass(o, me).wait_send()

    loop(n_chips, sent_meta, 1)
    meta_pass(0, me, meta_ref).wait_send()
    own_to_partner(me).wait_send()
    for g, ks in steps:
        for f, k in two(ks):
            link_copy(f, g, k, True).wait_send()
            pass_on(f, g, k, True).wait_send()
    x_out.wait()


def dispatch(ep, n_local, resid_in, expert_ids, priority, norm_gain, router_w, shared_w1, shared_w3, shared_w2):
    tok, dim = resid_in.shape
    top_k = expert_ids.shape[1]
    side = math.isqrt(ep // 2)
    n_exp = ep * n_local
    slots = tok * top_k + (n_local - 1) * TILE
    n_piece = 2 * (side + 1) * 4
    n_buf, width = 3, 256
    vmem = pl.BlockSpec(memory_space=pltpu.VMEM)
    hbm = pl.BlockSpec(memory_space=pl.ANY)
    dma = pltpu.SemaphoreType.DMA
    return pl.pallas_call(
        functools.partial(dispatch_kernel, ep, top_k, n_local),
        out_shape=(
            jax.ShapeDtypeStruct((slots, dim), BF16),
            jax.ShapeDtypeStruct((8, 128), jnp.int32),
            jax.ShapeDtypeStruct((n_exp, tok), jnp.int32),
            jax.ShapeDtypeStruct((n_exp, tok), F32),
            jax.ShapeDtypeStruct((tok, dim), F32),
        ),
        in_specs=[vmem] * 5 + [hbm] * 3,
        out_specs=(hbm, vmem, vmem, vmem, vmem),
        scratch_shapes=[
            pltpu.VMEM((slots, dim), BF16),
            pltpu.VMEM((tok, dim), BF16),
            pltpu.VMEM((2 * top_k, tok), jnp.int32),
            pltpu.VMEM((ep, tok, dim), BF16),
            pltpu.VMEM((ep, 2 * top_k, tok), jnp.int32),
            pltpu.VMEM((top_k, ep, tok), jnp.int32),
            pltpu.VMEM((top_k, ep, tok), jnp.int32),
            pltpu.VMEM((n_exp, ep, tok), jnp.int32),
            pltpu.VMEM((ep, tok), jnp.int32),
            pltpu.VMEM((ep, tok), F32),
            pltpu.VMEM((ep * ep, tok), F32),
            pltpu.VMEM((n_local, ep, tok), jnp.int32),
            pltpu.VMEM((n_exp, tok), F32),
            pltpu.VMEM((n_exp, tok), F32),
            pltpu.VMEM((slots, 4 * tok), BF16),
            pltpu.VMEM((n_buf, dim, width), BF16),
            pltpu.VMEM((n_buf, dim, width), BF16),
            pltpu.VMEM((n_buf, width, dim), BF16),
            dma(()), dma(()), dma((n_buf, 3)),
            dma((ep,)), dma((ep,)), dma((n_piece,)), dma((n_piece,)), dma((n_piece,)), dma((n_piece,)), dma(()), dma(()),
        ],
        compiler_params=pltpu.CompilerParams(collective_id=0, has_side_effects=True, vmem_limit_bytes=VMEM_LIMIT),
        name="dispatch",
    )(
        resid_in, expert_ids.T, priority.T, norm_gain.reshape(1, dim), router_w.T, shared_w1, shared_w3, shared_w2,
    )


def expert_kernel(
    ep, sc, x_hbm, w1_hbm, w3_hbm, w2_hbm, e_hbm, a_hbm, b_hbm, x_ref, e_ref, act, w1, w3, w2, bk, x_sem, e_sem, sems, bk_sem
):
    n_local, dim, ff = w1.shape
    slots = x_ref.shape[0]
    step = 4 * TILE
    parts = PARTS + ((PARTS[-1][1], ff),)
    last = len(parts)
    x_in = pltpu.make_async_copy(x_hbm, x_ref, x_sem)

    def loads(l, n):
        if n == last:
            return [pltpu.make_async_copy(w2_hbm.at[l], w2.at[l], sems.at[l, 2 * n])]
        cols = pl.ds(parts[n][0], parts[n][1] - parts[n][0])
        return [
            pltpu.make_async_copy(w_hbm.at[l, :, cols], w.at[l, :, cols], sems.at[l, 2 * n + i])
            for i, (w_hbm, w) in enumerate(((w1_hbm, w1), (w3_hbm, w3)))
        ]

    def request(l, n):
        l, n = (l, n) if n <= last else (l + 1, n - last - 1)

        @pl.when(l < n_local)
        def _():
            for load in loads(l, n):
                load.start()

    def arrive(l, n):
        for load in loads(l, n):
            load.wait()
        request(l, n + AHEAD)

    x_in.start()
    for n in range(AHEAD):
        request(0, n)

    def over_tiles(first, count, body):
        most = 4
        whole = count // most

        def many(i):
            body(pl.ds(pl.multiple_of((first + i * most) * TILE, TILE), most * TILE))

        loop(whole, many)
        for rest in range(1, most):

            @pl.when(lax.rem(count, most) == rest)
            def _():
                body(pl.ds(pl.multiple_of((first + whole * most) * TILE, TILE), rest * TILE))

    x_in.wait()

    def one_expert(l, done):
        count = (sc[2 * l + 1, ep - 1] - sc[2 * l + 1, 0] + sc[2 * l, ep - 1] + TILE - 1) // TILE

        def up_cols(n):
            start = pl.multiple_of(jnp.minimum(n * step, ff - step), TILE)
            for p, (c, _) in enumerate(parts):

                @pl.when(n * step == c)
                def _():
                    arrive(l, p)

            def up(rows):
                x = x_ref[rows, :]
                up_a = jnp.dot(x, w1[l, :, pl.ds(start, step)], preferred_element_type=F32)
                up_b = jnp.dot(x, w3[l, :, pl.ds(start, step)], preferred_element_type=F32)
                act[rows, pl.ds(start, step)] = (up_a * jax.nn.sigmoid(up_a) * up_b).astype(BF16)

            over_tiles(done, count, up)

        loop(-(-ff // step), up_cols)
        arrive(l, last)

        def down_cols(n):
            cols = pl.ds(pl.multiple_of(n * step, step), step)

            def down(rows):
                e_ref[rows, cols] = jnp.dot(act[rows, :], w2[l, :, cols], preferred_element_type=F32).astype(BF16)

            over_tiles(done, count, down)

        loop(dim // step, down_cols)
        return done + count

    done = lax.fori_loop(0, n_local, one_expert, 0)

    def clear(i):
        rows = pl.ds(pl.multiple_of(i * TILE, TILE), TILE)
        e_ref[rows, :] = jnp.zeros((TILE, dim), BF16)

    loop(slots // TILE, clear, done)
    e_out = pltpu.make_async_copy(e_ref, e_hbm, e_sem)
    e_out.start()
    fill_buckets(ep, sc, 0, e_ref, a_hbm, b_hbm, bk, bk_sem, n_local)
    e_out.wait()


def bucket_shape(ep, dim):
    side = math.isqrt(ep // 2)
    return jax.ShapeDtypeStruct((side, 2, side, CAP, dim // 4), BF16)


def bucket_scratch(ep, dim):
    n_chips = ep // 2
    return [pltpu.VMEM((n_chips, 4, CAP, dim // 4), BF16), pltpu.SemaphoreType.DMA((n_chips, 4))]


def experts(ep, info, x, expert_w1, expert_w3, expert_w2):
    hbm = pl.BlockSpec(memory_space=pl.ANY)
    n_local, dim, ff = expert_w1.shape
    bucket = bucket_shape(ep, dim)
    bk, bk_sem = bucket_scratch(ep, dim)
    dma = pltpu.SemaphoreType.DMA
    return pl.pallas_call(
        functools.partial(expert_kernel, ep),
        out_shape=(jax.ShapeDtypeStruct(x.shape, BF16), bucket, bucket),
        in_specs=[pl.BlockSpec(memory_space=pltpu.SMEM)] + [hbm] * 4,
        out_specs=(hbm, hbm, hbm),
        scratch_shapes=[
            pltpu.VMEM(x.shape, BF16),
            pltpu.VMEM(x.shape, BF16),
            pltpu.VMEM((x.shape[0], ff), BF16),
            pltpu.VMEM((n_local, dim, ff), BF16),
            pltpu.VMEM((n_local, dim, ff), BF16),
            pltpu.VMEM((n_local, ff, dim), BF16),
            bk, dma(()), dma(()), dma((n_local, 2 * len(PARTS) + 3)), bk_sem,
        ],
        compiler_params=pltpu.CompilerParams(vmem_limit_bytes=VMEM_LIMIT),
        name="experts",
    )(info, x, expert_w1, expert_w3, expert_w2)


def fill_kernel(ep, n_local, sc, rnd, e_ref, a_hbm, b_hbm, bk, bk_sem):
    fill_buckets(ep, sc, rnd[0], e_ref, a_hbm, b_hbm, bk, bk_sem, n_local)


def fill_buckets(ep, sc, rnd, e_ref, a_hbm, b_hbm, bk, bk_sem, n_local):
    pc = Place(ep)
    side = pc.side
    slots, dim = e_ref.shape
    width = dim // 4
    pack = 16
    window = (CAP + 2 * pack - 2) // pack * pack
    skip = rnd * CAP

    def out_copies(n):
        dx, dy = lax.rem(n, side), n // side
        targets = [a_hbm.at[dx, c, dy] for c in PAIR] + [b_hbm.at[dy, c, dx] for c in PAIR]
        return [pltpu.make_async_copy(bk.at[n, c], target, bk_sem.at[n, c]) for c, target in enumerate(targets)]

    def one(n):
        dx, dy = lax.rem(n, side), n // side
        chip = lax.rem(pc.py + dy, side) * side + lax.rem(pc.px + dx, side)
        row = iota((CAP, window), 0)
        col = iota((CAP, window), 1)
        out = jnp.zeros((CAP, dim), F32)
        lead = -skip
        for l in range(n_local):
            start, count = sc[2 * l + 1, 2 * chip], sc[2 * l, 2 * chip] + sc[2 * l, 2 * chip + 1]
            used = jnp.minimum(jnp.maximum(-lead, 0), count)
            origin = jnp.minimum((start + used) // pack * pack, slots - window)
            origin = pl.multiple_of(origin, pack)
            slot = row - lead + start
            hit = (slot == col + origin) & (row >= lead) & (row < lead + count)
            out = out + jnp.dot(jnp.where(hit, 1.0, 0.0).astype(BF16), e_ref[pl.ds(origin, window), :], preferred_element_type=F32)
            lead = lead + count
        out = out.astype(BF16)
        for c, copy in enumerate(out_copies(n)):
            bk[n, c] = out[:, c * width : (c + 1) * width]
            copy.start()

    def sent(n):
        for copy in out_copies(n):
            copy.wait()

    loop(side * side, one, unroll=4)
    loop(side * side, sent)


def fill(ep, n_local, info, rnd, e):
    vmem = pl.BlockSpec(memory_space=pltpu.VMEM)
    smem = pl.BlockSpec(memory_space=pltpu.SMEM)
    hbm = pl.BlockSpec(memory_space=pl.ANY)
    bucket = bucket_shape(ep, e.shape[1])
    return pl.pallas_call(
        functools.partial(fill_kernel, ep, n_local),
        out_shape=(bucket, bucket),
        in_specs=[smem, smem, vmem],
        out_specs=(hbm, hbm),
        scratch_shapes=bucket_scratch(ep, e.shape[1]),
        compiler_params=pltpu.CompilerParams(vmem_limit_bytes=VMEM_LIMIT),
        name="fill",
    )(info, rnd, e)


def combine_kernel(
    ep, n_local, a_hbm, b_hbm, q_ref, p_ref, acc_ref, out_ref, bk, st, rl, fin, ry, pf, g_ref, bk_sem, s_send, s_recv, p_send, p_recv
):
    pc = Place(ep)
    side = pc.side
    tok = q_ref.shape[1]
    width = bk.shape[-1]
    loads = [pltpu.make_async_copy(src, bk.at[fam], bk_sem.at[fam]) for fam, src in enumerate((a_hbm, b_hbm))]
    for load in loads:
        load.start()

    barrier = pltpu.get_barrier_semaphore()
    friends = [pc.dev(1, 0), pc.dev(-1, 0), pc.dev(0, 1), pc.dev(0, -1), pc.partner]
    for friend in friends:
        pl.semaphore_signal(barrier, inc=1, device_id={"ep": friend}, device_id_type=MESH)
    pl.semaphore_wait(barrier, len(friends))
    for load in loads:
        load.wait()

    ring = (0, 1, side - 1, 2)

    def held(fam, j):
        return bk.at[fam, 0] if j == 0 else st.at[fam, j]

    def link_copy(fam, g, k):
        hop = 1 if k % 2 == 0 else -1
        c = k % 2
        if g == 0:
            target = pc.at(fam, hop, 0)
            if k < 2:
                src, dst = bk.at[fam, hop % side], st.at[fam, hop % side]
            elif k < 4:
                src, dst = bk.at[fam, 2, c], rl.at[fam, c]
            else:
                src, dst = rl.at[fam, c], st.at[fam, 2, c]
        else:
            j = g - 1
            target = pc.at(fam, 0, hop)
            if k < 2:
                src, dst = held(fam, j).at[:, hop % side], fin.at[fam, j, hop % side]
            elif k < 4:
                src, dst = held(fam, j).at[c, 2], ry.at[fam, j, c]
            else:
                src, dst = ry.at[fam, j, c], fin.at[fam, j, 2, c]
        n = (fam * (side + 1) + g) * 6 + k
        return pltpu.make_async_remote_copy(
            src_ref=src, dst_ref=dst, send_sem=s_send.at[n], recv_sem=s_recv.at[n], device_id={"ep": target}, device_id_type=MESH
        )

    def arrived(fam, j, v):
        return held(fam, j).at[:, 0] if v == 0 else fin.at[fam, j, v]

    def pass_on(fam, j, v):
        n = (fam * side + j) * side + v
        return pltpu.make_async_remote_copy(
            src_ref=arrived(fam, j, v), dst_ref=pf.at[fam, j, v], send_sem=p_send.at[n], recv_sem=p_recv.at[n],
            device_id={"ep": pc.partner}, device_id_type=MESH,
        )

    for k in SENDS:
        for fam in PAIR:
            link_copy(fam, 0, k).start()
    for k in SENDS:
        for fam in PAIR:
            link_copy(fam, 1, k).start()
    for fam in PAIR:
        pass_on(fam, 0, 0).start()

    row = iota((g_ref.shape[3], tok), 0)

    def weights(d):
        w = jnp.zeros(row.shape, F32)
        for l in range(n_local):
            e = d * n_local + l
            w = w + jnp.where(row == q_ref[pl.ds(e, 1), :], p_ref[pl.ds(e, 1), :], 0.0)
        w = w.T
        for n in range(3):
            term = w.astype(BF16)
            g_ref[d, n] = term
            w = w - term.astype(F32)

    loop(ep, weights)
    out_ref[...] = acc_ref[...]

    def add(fam, j, v):
        devs = [pc.at(fam, -j, -v), pc.at(fam, -j, -v, 1 - pc.core)]

        def one(c):
            cols = pl.ds(pl.multiple_of((2 * fam + c) * width, width), width)
            total = out_ref[:, cols]
            for d, rows in zip(devs, (arrived(fam, j, v), pf.at[fam, j, v])):
                data = rows[c]
                for n in range(3):
                    total = total + jnp.dot(g_ref[d, n][:, :CAP], data, preferred_element_type=F32)
            out_ref[:, cols] = total

        loop(2, one, unroll=2)

    ready = []

    def here(fam, j, v):
        pass_on(fam, j, v).start()
        ready.append((fam, j, v))

    def drain(keep):
        while len(ready) > keep:
            fam, j, v = ready.pop(0)
            pass_on(fam, j, v).wait_recv()
            add(fam, j, v)

    def got(fam, g, k):
        link_copy(fam, g, k).wait_recv()

    ready += [(0, 0, 0), (1, 0, 0)]
    for k in SPLIT:
        for fam in PAIR:
            got(fam, 0, k)
            link_copy(fam, 0, k + 2).start()
    drain(0)
    for k in PAIR:
        for fam in PAIR:
            got(fam, 0, k)
            j = 1 if k == 0 else side - 1
            for kk in SENDS:
                link_copy(fam, 1 + j, kk).start()
            here(fam, j, 0)
    for k in SPLIT:
        for fam in PAIR:
            got(fam, 1, k)
            link_copy(fam, 1, k + 2).start()
    for fam in PAIR:
        got(fam, 0, 4)
        got(fam, 0, 5)
        for kk in SENDS:
            link_copy(fam, 3, kk).start()
        here(fam, 2, 0)
    drain(2)
    for j in ring:
        if j > 0:
            for k in SPLIT:
                for fam in PAIR:
                    got(fam, 1 + j, k)
                    link_copy(fam, 1 + j, k + 2).start()
        for k in PAIR:
            for fam in PAIR:
                got(fam, 1 + j, k)
                here(fam, j, 1 if k == 0 else side - 1)
        drain(2)
    for j in ring:
        for fam in PAIR:
            got(fam, 1 + j, 4)
            got(fam, 1 + j, 5)
            here(fam, j, 2)
        drain(4)
    drain(0)
    for fam in PAIR:
        for g in range(side + 1):
            for k in range(6):
                link_copy(fam, g, k).wait_send()
        for j in range(side):
            for v in range(side):
                pass_on(fam, j, v).wait_send()


def combine(ep, n_local, bka, bkb, q, weights, acc):
    side = math.isqrt(ep // 2)
    cap, width = bka.shape[-2:]
    tok = q.shape[1]
    vmem = pl.BlockSpec(memory_space=pltpu.VMEM)
    hbm = pl.BlockSpec(memory_space=pl.ANY)
    dma = pltpu.SemaphoreType.DMA
    n_link, n_pass = 2 * (side + 1) * 6, 2 * side * side
    return pl.pallas_call(
        functools.partial(combine_kernel, ep, n_local),
        out_shape=jax.ShapeDtypeStruct(acc.shape, F32),
        in_specs=[hbm, hbm, vmem, vmem, vmem],
        out_specs=vmem,
        scratch_shapes=[
            pltpu.VMEM((2, side, 2, side, cap, width), BF16),
            pltpu.VMEM((2, side, 2, side, cap, width), BF16),
            pltpu.VMEM((2, 2, side, cap, width), BF16),
            pltpu.VMEM((2, side, side, 2, cap, width), BF16),
            pltpu.VMEM((2, side, 2, cap, width), BF16),
            pltpu.VMEM((2, side, side, 2, cap, width), BF16),
            pltpu.VMEM((ep, 3, tok, tok), BF16),
            dma((2,)), dma((n_link,)), dma((n_link,)), dma((n_pass,)), dma((n_pass,)),
        ],
        compiler_params=pltpu.CompilerParams(collective_id=1, has_side_effects=True, vmem_limit_bytes=VMEM_LIMIT),
        name="combine",
    )(bka, bkb, q, weights, acc)


def solution(mesh):
    ep = mesh.shape["ep"]
    tok_spec = P(("dp", "ep"))
    expert_spec = P("ep")

    def device_fn(resid_in, expert_ids, priority, norm_gain, router_w, shared_w1, shared_w3, shared_w2, expert_w1, expert_w3, expert_w2):
        n_local = expert_w1.shape[0]
        x, info, q, gates, base = dispatch(
            ep, n_local, resid_in, expert_ids, priority, norm_gain, router_w, shared_w1, shared_w3, shared_w2
        )
        e, bka, bkb = experts(ep, info, x, expert_w1, expert_w3, expert_w2)
        first = combine(ep, n_local, bka, bkb, q, gates, base)
        rounds = lax.div(info[2 * n_local, 0] + (CAP - 1), CAP)

        def one_round(carry):
            rnd, acc = carry
            more_a, more_b = fill(ep, n_local, info, rnd[None], e)
            return rnd + 1, combine(ep, n_local, more_a, more_b, q - rnd * CAP, gates, acc)

        total = lax.while_loop(lambda carry: carry[0] < rounds, one_round, (jnp.int32(1), first))[1]
        return total.astype(BF16)

    return jax.shard_map(
        device_fn, mesh=mesh,
        in_specs=(tok_spec, tok_spec, tok_spec, P(), P(), P(), P(), P(), expert_spec, expert_spec, expert_spec),
        out_specs=tok_spec, check_vma=False,
    )
```

```python
import functools
import math

import jax
import jax.numpy as jnp
from jax import lax
from jax.experimental import pallas as pl
from jax.experimental.pallas import tpu as pltpu
from jax.sharding import PartitionSpec as P

NORM_EPS = 1e-6
ROUTE_SCALE = 16.0
MESH = pl.DeviceIdType.MESH
F32 = jnp.float32
BF16 = jnp.bfloat16
PAIR = (0, 1)
SPLIT = (2, 3)
SENDS = SPLIT + PAIR
LANES = (((1,), (1,)), ((), ()))
FAR = 1 << 20
TILE = 64
PARTS = ((0, 512), (512, 1024))
AHEAD = 2
CAP = 72
VMEM_LIMIT = 64000 * 1024


class Place:
    def __init__(self, ep):
        self.side = math.isqrt(ep // 2)
        self.me = lax.axis_index("ep")
        self.core = lax.rem(self.me, 2)
        self.chip = self.me // 2
        self.px = lax.rem(self.chip, self.side)
        self.py = self.chip // self.side
        self.partner = self.me + 1 - 2 * self.core

    def dev(self, dx, dy, core=None):
        x = lax.rem(self.px + dx % self.side, self.side)
        y = lax.rem(self.py + dy % self.side, self.side)
        return (y * self.side + x) * 2 + (self.core if core is None else core)

    def at(self, fam, du, dv, core=None):
        return self.dev(du, dv, core) if fam == 0 else self.dev(dv, du, core)


def loop(n, body, start=0, unroll=1):
    def step(i, carry):
        body(i)
        return carry

    lax.fori_loop(start, n, step, 0, unroll=unroll)


def iota(shape, axis):
    return lax.broadcasted_iota(jnp.int32, shape, axis)


def tri(n, m, rows_first):
    i = iota((n, m), 0)
    j = iota((n, m), 1)
    return jnp.where(i < j if rows_first else j < i, 1.0, 0.0).astype(BF16)


def mm(a, b):
    return jnp.dot(a.astype(BF16), b.astype(BF16), preferred_element_type=F32)


def mm_t(a, b):
    return lax.dot_general(a.astype(BF16), b.astype(BF16), LANES, preferred_element_type=F32)


def route(pc, ep, top_k, n_local, n_chips, meta_all, ids, prs, pr, thr, cnt, kch, pos, ka, kb, info_ref, q_ref):
    n_exp = ep * n_local
    tok = ids.shape[2]
    capacity = tok * top_k
    n_bits = (ep * capacity).bit_length()

    def unpack(s):
        for k in range(top_k):
            ids[k, pl.ds(s, 1), :] = meta_all[s, k : k + 1, :]
            prs[k, pl.ds(s, 1), :] = meta_all[s, top_k + k : top_k + k + 1, :]

    loop(ep, unpack)

    def per_expert(e):
        best = jnp.full((ep, tok), FAR, jnp.int32)
        for k in range(top_k):
            best = jnp.minimum(best, jnp.where(ids[k] == e, prs[k], FAR))
        pr[e] = best

    loop(n_exp, per_expert)

    thr[...] = jnp.zeros(thr.shape, jnp.int32)

    def bit_step(i, step):
        for d in range(ep):
            cand = thr[d : d + 1, :] + step
            hits = jnp.zeros((ep, tok), F32)
            for l in range(n_local):
                hits = hits + jnp.where(pr[d * n_local + l] < cand, 1.0, 0.0)
            cnt[d : d + 1, :] = jnp.sum(hits, axis=0, keepdims=True)
        total = jnp.sum(cnt[...], axis=1, keepdims=True)
        thr[...] = thr[...] + jnp.where(total <= capacity, step, 0)
        return step // 2

    lax.fori_loop(0, n_bits, bit_step, jnp.int32(1 << (n_bits - 1)))

    def chip_counts(d):
        kept = jnp.zeros((ep, tok), F32)
        for l in range(n_local):
            kept = kept + jnp.where(pr[d * n_local + l] < thr[pl.ds(d, 1), :], 1.0, 0.0)
        kch[pl.ds(pl.multiple_of(d * ep, ep), ep), :] = kept

    loop(ep, chip_counts)
    pairs = kch[pl.ds(0, ep * n_chips, stride=2), :] + kch[pl.ds(1, ep * n_chips, stride=2), :]
    worst = jnp.max(jnp.sum(pairs, axis=1, keepdims=True), axis=0, keepdims=True)
    info_ref[...] = jnp.broadcast_to(worst, info_ref.shape).astype(jnp.int32)
    upper = tri(tok, tok, True)
    ones = jnp.ones((tok, tok), BF16)
    lower = tri(ep, ep, False)
    my_thr = thr[pl.ds(pc.me, 1), :]
    base = jnp.zeros((1, tok), F32)
    for l in range(n_local):
        kept = pr[pc.me * n_local + l] < my_thr
        kept_f = jnp.where(kept, 1.0, 0.0)
        in_row = mm(kept_f, upper)
        row_total = mm(kept_f, ones)
        row_start = mm(lower, row_total)
        pos[l] = jnp.where(kept, (in_row + row_start + base), -1.0).astype(jnp.int32)
        totals = mm_t(jnp.ones((8, tok), F32), kept_f)
        starts = mm(totals, tri(ep, ep, True)) + base[:, :ep]
        info_ref[2 * l : 2 * l + 1, :ep] = totals[:1].astype(jnp.int32)
        info_ref[2 * l + 1 : 2 * l + 2, :ep] = starts[:1].astype(jnp.int32)
        group = jnp.sum(row_total, axis=0, keepdims=True)
        base = base + jnp.floor((group + (TILE - 1)) * (1.0 / TILE)) * TILE

    def chip_rows(e):
        limit = thr[pl.ds(e // n_local, 1), :]
        first = pr[e, pl.ds(pc.chip * 2, 1), :]
        second = pr[e, pl.ds(pc.chip * 2 + 1, 1), :]
        ka[pl.ds(e, 1), :] = jnp.where(first < limit, 1.0, 0.0)
        kb[pl.ds(e, 1), :] = jnp.where(second < limit, 1.0, 0.0)

    loop(n_exp, chip_rows)
    k_a, k_b = ka[...], kb[...]
    tot_a = mm(k_a, ones)
    both = tot_a + mm(k_b, ones)
    i = iota((n_exp, n_exp), 0)
    j = iota((n_exp, n_exp), 1)
    earlier = jnp.where((j < i) & (j // n_local == i // n_local), 1.0, 0.0)
    before = mm(earlier, both)
    q_a = jnp.where(k_a > 0, mm(k_a, upper) + before, -1.0)
    q_b = jnp.where(k_b > 0, mm(k_b, upper) + tot_a + before, -1.0)
    second_core = iota(q_ref.shape, 0) * 0 + pc.core
    q_ref[...] = jnp.where(second_core == 0, q_a, q_b).astype(jnp.int32)


def dispatch_kernel(
    ep, top_k, n_local, y_ref, ids_ref, prio_ref, gain_ref, router_ref, sw1_hbm, sw3_hbm, sw2_hbm,
    x_hbm, info_ref, q_ref, gate_ref, base_ref,
    x_ref, b_ref, meta_ref, yall, meta_all, ids, prs, pr, thr, cnt, kch, pos, ka, kb, sel, sw1, sw3, sw2,
    own_sem, x_sem, sw_sem, m_send, m_recv, s_send, s_recv, p_send, p_recv, o_send, o_recv,
):
    pc = Place(ep)
    side, me = pc.side, pc.me
    tok, dim = y_ref.shape
    half, quarter, n_chips = tok // 2, tok // 4, ep // 2
    n_buf, width = sw1.shape[0], sw1.shape[2]
    n_chunks = sw1_hbm.shape[1] // width

    def shared_loads(c):
        slot = lax.rem(c, n_buf)
        cols = pl.ds(pl.multiple_of(c * width, width), width)
        return [
            pltpu.make_async_copy(sw1_hbm.at[:, cols], sw1.at[slot], sw_sem.at[slot, 0]),
            pltpu.make_async_copy(sw3_hbm.at[:, cols], sw3.at[slot], sw_sem.at[slot, 1]),
            pltpu.make_async_copy(sw2_hbm.at[cols, :], sw2.at[slot], sw_sem.at[slot, 2]),
        ]

    def first_loads(c):
        for load in shared_loads(c):
            load.start()

    loop(n_buf, first_loads)

    meta_ref[0:top_k, :] = ids_ref[...]
    meta_ref[top_k:, :] = prio_ref[...]

    def norm(i):
        rows = pl.ds(pl.multiple_of(i * 16, 16), 16)
        y = y_ref[rows, :].astype(F32)
        inv_rms = lax.rsqrt(jnp.mean(y * y, axis=1, keepdims=True) + NORM_EPS)
        b_ref[rows, :] = (y * inv_rms * gain_ref[...]).astype(BF16)

    loop(tok // 16, norm)

    barrier = pltpu.get_barrier_semaphore()

    def greet(o):
        pl.semaphore_signal(barrier, inc=1, device_id={"ep": lax.rem(me + 2 * o, ep)}, device_id_type=MESH)

    loop(n_chips, greet, 1)
    pl.semaphore_signal(barrier, inc=1, device_id={"ep": pc.partner}, device_id_type=MESH)
    pl.semaphore_wait(barrier, n_chips)

    own = pltpu.make_async_copy(b_ref, yall.at[me], own_sem)
    own.start()

    def meta_copy(o, src):
        return pltpu.make_async_remote_copy(
            src_ref=meta_ref, dst_ref=meta_all.at[src], send_sem=m_send.at[o], recv_sem=m_recv.at[o],
            device_id={"ep": lax.rem(me + 2 * o, ep)}, device_id_type=MESH,
        )

    def meta_pass(o, origin, src=None):
        block = lax.rem(origin - 2 * o + ep, ep)
        return pltpu.make_async_remote_copy(
            src_ref=meta_all.at[block] if src is None else src, dst_ref=meta_all.at[block],
            send_sem=m_send.at[n_chips + o], recv_sem=m_recv.at[n_chips + o], device_id={"ep": pc.partner}, device_id_type=MESH,
        )

    def send_meta(o):
        meta_copy(o, me).start()

    loop(n_chips, send_meta, 1)
    meta_pass(0, me, meta_ref).start()

    def piece(fam, g, k, sent):
        j = g - 1
        hop = -1 if k % 2 else 1
        dist = (0 if sent else -hop) if k in PAIR else (-hop if sent else 2)
        du, dv = (dist, 0) if g == 0 else (j, dist)
        start = fam * half + (quarter if k == 3 else 0)
        size = half if k < 2 else quarter
        return du % side, dv % side, start, size, hop

    def link_copy(fam, g, k, sent):
        du, dv, start, size, hop = piece(fam, g, k, sent)
        block = pc.at(fam, du, dv)
        rows = yall.at[block, pl.ds(start, size), :]
        source = b_ref.at[pl.ds(start, size), :] if sent and (du, dv) == (0, 0) else rows
        target = pc.at(fam, hop, 0) if g == 0 else pc.at(fam, 0, hop)
        n = (fam * (side + 1) + g) * 4 + k
        return pltpu.make_async_remote_copy(
            src_ref=source, dst_ref=rows, send_sem=s_send.at[n], recv_sem=s_recv.at[n], device_id={"ep": target}, device_id_type=MESH
        )

    def pass_on(fam, g, k, mine):
        du, dv, start, size, _ = piece(fam, g, k, False)
        block = pc.at(fam, du, dv, pc.core if mine else 1 - pc.core)
        rows = yall.at[block, pl.ds(start, size), :]
        n = (fam * (side + 1) + g) * 4 + k
        return pltpu.make_async_remote_copy(
            src_ref=rows, dst_ref=rows, send_sem=p_send.at[n], recv_sem=p_recv.at[n], device_id={"ep": pc.partner}, device_id_type=MESH
        )

    def own_to_partner(block):
        return pltpu.make_async_remote_copy(
            src_ref=b_ref, dst_ref=yall.at[block], send_sem=o_send, recv_sem=o_recv, device_id={"ep": pc.partner}, device_id_type=MESH
        )

    for fam in PAIR:
        for k in PAIR:
            link_copy(fam, 0, k, True).start()
    own_to_partner(me).start()
    for fam in PAIR:
        for k in PAIR:
            link_copy(fam, 1, k, True).start()

    def wait_meta(o):
        meta_copy(o, lax.rem(me - 2 * o + ep, ep)).wait_recv()
        meta_pass(o, me).start()

    def wait_passed(o):
        meta_pass(o, pc.partner).wait_recv()

    def gates():
        logits = lax.dot_general(router_ref[...], b_ref[...], LANES, preferred_element_type=F32)
        probs = jnp.exp(logits - jnp.max(logits, axis=0, keepdims=True))
        gate_ref[...] = ROUTE_SCALE * (probs / jnp.sum(probs, axis=0, keepdims=True))

    def shared(c):
        slot = lax.rem(c, n_buf)
        for load in shared_loads(c):
            load.wait()
        up_a = jnp.dot(b_ref[...], sw1[slot], preferred_element_type=F32)
        up_b = jnp.dot(b_ref[...], sw3[slot], preferred_element_type=F32)
        act = (up_a * jax.nn.sigmoid(up_a) * up_b).astype(BF16)
        base_ref[...] += jnp.dot(act, sw2[slot], preferred_element_type=F32)

        @pl.when(c + n_buf < n_chunks)
        def _():
            for load in shared_loads(c + n_buf):
                load.start()

    base_ref[...] = jnp.zeros(base_ref.shape, F32)
    shared_done = [0]

    def fill_in(n):
        end = min(shared_done[0] + n, n_chunks)
        if end > shared_done[0]:
            loop(end, shared, shared_done[0])
        shared_done[0] = end

    meta_all[me] = meta_ref[...]
    gates()
    loop(n_chips, wait_meta, 1)
    loop(n_chips, wait_passed)
    route(pc, ep, top_k, n_local, n_chips, meta_all, ids, prs, pr, thr, cnt, kch, pos, ka, kb, info_ref, q_ref)

    slots = x_ref.shape[0]
    n_cols = 512
    lane = iota((1, tok), 1)

    def pick(halves, first=False):
        depth = len(halves) * tok
        where_to = [[jnp.where(lane < half, pos[l, pl.ds(lo, 1), :], pos[l, pl.ds(hi, 1), :]) for l in range(n_local)] for lo, hi in halves]

        def build(i):
            rows = pl.ds(pl.multiple_of(i * TILE, TILE), TILE)
            slot = iota((TILE, tok), 0) + i * TILE
            for n, places in enumerate(where_to):
                hit = slot == places[0]
                for place in places[1:]:
                    hit = hit | (slot == place)
                sel[rows, n * tok : (n + 1) * tok] = jnp.where(hit, 1.0, 0.0).astype(BF16)

        loop(slots // TILE, build)

        def one(n):
            cols = pl.ds(pl.multiple_of(n * n_cols, n_cols), n_cols)
            pieces = []
            for lo, hi in halves:
                pieces += [yall[lo, :half, cols], yall[hi, half:, cols]]
            picked = jnp.dot(sel[:, :depth], jnp.concatenate(pieces, axis=0), preferred_element_type=F32).astype(BF16)
            x_ref[:, cols] = picked if first else x_ref[:, cols] + picked

        loop(dim // n_cols, one)

    def two(ks):
        return [(f, k) for f in PAIR for k in ks]

    steps = [(0, PAIR), (1, PAIR), (0, SPLIT), (side, PAIR), (2, PAIR), (1, SPLIT), (3, PAIR)]
    steps += [(g, SPLIT) for g in (side, 2, 3)]

    def receive(g, ks):
        for f, k in two(ks):
            link_copy(f, g, k, False).wait_recv()
            if k < 2:
                link_copy(f, g, k + 2, True).start()
        if g == 0:
            for j in (side - 1, 1) if ks == PAIR else (2,):
                for f, k in two(PAIR):
                    link_copy(f, 1 + j, k, True).start()
        for f, k in two(ks):
            pass_on(f, g, k, True).start()

    def take(g, ks):
        for f, k in two(ks):
            pass_on(f, g, k, False).wait_recv()
        halves = []
        for k in ks if ks == PAIR else (2,):
            for core in (pc.core, 1 - pc.core):
                halves.append(tuple(pc.at(f, *piece(f, g, k, False)[:2], core) for f in PAIR))
        pick(halves)

    own.wait()
    own_to_partner(pc.partner).wait_recv()
    pick([(me, me), (pc.partner, pc.partner)], first=True)
    for i, step in enumerate(steps):
        receive(*step)
        if i > 0:
            take(*steps[i - 1])
        if i in (1, 3, 4, 6):
            fill_in(3)
    take(*steps[-1])
    x_out = pltpu.make_async_copy(x_ref, x_hbm, x_sem)
    x_out.start()
    base_ref[...] = y_ref[...].astype(F32) + base_ref[...].astype(BF16).astype(F32)

    def sent_meta(o):
        meta_copy(o, me).wait_send()
        meta_pass(o, me).wait_send()

    loop(n_chips, sent_meta, 1)
    meta_pass(0, me, meta_ref).wait_send()
    own_to_partner(me).wait_send()
    for g, ks in steps:
        for f, k in two(ks):
            link_copy(f, g, k, True).wait_send()
            pass_on(f, g, k, True).wait_send()
    x_out.wait()


def dispatch(ep, n_local, resid_in, expert_ids, priority, norm_gain, router_w, shared_w1, shared_w3, shared_w2):
    tok, dim = resid_in.shape
    top_k = expert_ids.shape[1]
    side = math.isqrt(ep // 2)
    n_exp = ep * n_local
    slots = tok * top_k + (n_local - 1) * TILE
    n_piece = 2 * (side + 1) * 4
    n_buf, width = 3, 256
    vmem = pl.BlockSpec(memory_space=pltpu.VMEM)
    hbm = pl.BlockSpec(memory_space=pl.ANY)
    dma = pltpu.SemaphoreType.DMA
    return pl.pallas_call(
        functools.partial(dispatch_kernel, ep, top_k, n_local),
        out_shape=(
            jax.ShapeDtypeStruct((slots, dim), BF16),
            jax.ShapeDtypeStruct((8, 128), jnp.int32),
            jax.ShapeDtypeStruct((n_exp, tok), jnp.int32),
            jax.ShapeDtypeStruct((n_exp, tok), F32),
            jax.ShapeDtypeStruct((tok, dim), F32),
        ),
        in_specs=[vmem] * 5 + [hbm] * 3,
        out_specs=(hbm, vmem, vmem, vmem, vmem),
        scratch_shapes=[
            pltpu.VMEM((slots, dim), BF16),
            pltpu.VMEM((tok, dim), BF16),
            pltpu.VMEM((2 * top_k, tok), jnp.int32),
            pltpu.VMEM((ep, tok, dim), BF16),
            pltpu.VMEM((ep, 2 * top_k, tok), jnp.int32),
            pltpu.VMEM((top_k, ep, tok), jnp.int32),
            pltpu.VMEM((top_k, ep, tok), jnp.int32),
            pltpu.VMEM((n_exp, ep, tok), jnp.int32),
            pltpu.VMEM((ep, tok), jnp.int32),
            pltpu.VMEM((ep, tok), F32),
            pltpu.VMEM((ep * ep, tok), F32),
            pltpu.VMEM((n_local, ep, tok), jnp.int32),
            pltpu.VMEM((n_exp, tok), F32),
            pltpu.VMEM((n_exp, tok), F32),
            pltpu.VMEM((slots, 4 * tok), BF16),
            pltpu.VMEM((n_buf, dim, width), BF16),
            pltpu.VMEM((n_buf, dim, width), BF16),
            pltpu.VMEM((n_buf, width, dim), BF16),
            dma(()), dma(()), dma((n_buf, 3)),
            dma((ep,)), dma((ep,)), dma((n_piece,)), dma((n_piece,)), dma((n_piece,)), dma((n_piece,)), dma(()), dma(()),
        ],
        compiler_params=pltpu.CompilerParams(collective_id=0, has_side_effects=True, vmem_limit_bytes=VMEM_LIMIT),
        name="dispatch",
    )(
        resid_in, expert_ids.T, priority.T, norm_gain.reshape(1, dim), router_w.T, shared_w1, shared_w3, shared_w2,
    )


def expert_kernel(
    ep, sc, x_hbm, w1_hbm, w3_hbm, w2_hbm, e_hbm, a_hbm, b_hbm, x_ref, e_ref, act, w1, w3, w2, bk, x_sem, e_sem, sems, bk_sem
):
    n_local, dim, ff = w1.shape
    slots = x_ref.shape[0]
    step = 8 * TILE
    parts = PARTS + ((PARTS[-1][1], ff),)
    last = len(parts)
    x_in = pltpu.make_async_copy(x_hbm, x_ref, x_sem)

    def loads(l, n):
        if n == last:
            return [pltpu.make_async_copy(w2_hbm.at[l], w2.at[l], sems.at[l, 2 * n])]
        cols = pl.ds(parts[n][0], parts[n][1] - parts[n][0])
        return [
            pltpu.make_async_copy(w_hbm.at[l, :, cols], w.at[l, :, cols], sems.at[l, 2 * n + i])
            for i, (w_hbm, w) in enumerate(((w1_hbm, w1), (w3_hbm, w3)))
        ]

    def request(l, n):
        l, n = (l, n) if n <= last else (l + 1, n - last - 1)

        @pl.when(l < n_local)
        def _():
            for load in loads(l, n):
                load.start()

    def arrive(l, n):
        for load in loads(l, n):
            load.wait()
        request(l, n + AHEAD)

    x_in.start()
    for n in range(AHEAD):
        request(0, n)

    def over_tiles(first, count, body):
        most = 6
        whole = count // most

        def many(i):
            body(pl.ds(pl.multiple_of((first + i * most) * TILE, TILE), most * TILE))

        loop(whole, many)
        for rest in range(1, most):

            @pl.when(lax.rem(count, most) == rest)
            def _():
                body(pl.ds(pl.multiple_of((first + whole * most) * TILE, TILE), rest * TILE))

    x_in.wait()

    def one_expert(l, done):
        count = (sc[2 * l + 1, ep - 1] - sc[2 * l + 1, 0] + sc[2 * l, ep - 1] + TILE - 1) // TILE

        def up_cols(n):
            start = pl.multiple_of(jnp.minimum(n * step, ff - step), 2 * TILE)
            for p, (c, _) in enumerate(parts):

                @pl.when(n * step == c)
                def _():
                    arrive(l, p)

            def up(rows):
                x = x_ref[rows, :]
                up_a = jnp.dot(x, w1[l, :, pl.ds(start, step)], preferred_element_type=F32)
                up_b = jnp.dot(x, w3[l, :, pl.ds(start, step)], preferred_element_type=F32)
                act[rows, pl.ds(start, step)] = (up_a * jax.nn.sigmoid(up_a) * up_b).astype(BF16)

            over_tiles(done, count, up)

        loop(-(-ff // step), up_cols)
        arrive(l, last)

        def down_cols(n):
            cols = pl.ds(pl.multiple_of(n * step, step), step)

            def down(rows):
                e_ref[rows, cols] = jnp.dot(act[rows, :], w2[l, :, cols], preferred_element_type=F32).astype(BF16)

            over_tiles(done, count, down)

        loop(dim // step, down_cols)
        return done + count

    done = lax.fori_loop(0, n_local, one_expert, 0)

    def clear(i):
        rows = pl.ds(pl.multiple_of(i * TILE, TILE), TILE)
        e_ref[rows, :] = jnp.zeros((TILE, dim), BF16)

    loop(slots // TILE, clear, done)
    e_out = pltpu.make_async_copy(e_ref, e_hbm, e_sem)
    e_out.start()
    fill_buckets(ep, sc, 0, e_ref, a_hbm, b_hbm, bk, bk_sem, n_local)
    e_out.wait()


def bucket_shape(ep, dim):
    side = math.isqrt(ep // 2)
    return jax.ShapeDtypeStruct((side, 2, side, CAP, dim // 4), BF16)


def bucket_scratch(ep, dim):
    n_chips = ep // 2
    return [pltpu.VMEM((n_chips, 4, CAP, dim // 4), BF16), pltpu.SemaphoreType.DMA((n_chips, 4))]


def experts(ep, info, x, expert_w1, expert_w3, expert_w2):
    hbm = pl.BlockSpec(memory_space=pl.ANY)
    n_local, dim, ff = expert_w1.shape
    bucket = bucket_shape(ep, dim)
    bk, bk_sem = bucket_scratch(ep, dim)
    dma = pltpu.SemaphoreType.DMA
    return pl.pallas_call(
        functools.partial(expert_kernel, ep),
        out_shape=(jax.ShapeDtypeStruct(x.shape, BF16), bucket, bucket),
        in_specs=[pl.BlockSpec(memory_space=pltpu.SMEM)] + [hbm] * 4,
        out_specs=(hbm, hbm, hbm),
        scratch_shapes=[
            pltpu.VMEM(x.shape, BF16),
            pltpu.VMEM(x.shape, BF16),
            pltpu.VMEM((x.shape[0], ff), BF16),
            pltpu.VMEM((n_local, dim, ff), BF16),
            pltpu.VMEM((n_local, dim, ff), BF16),
            pltpu.VMEM((n_local, ff, dim), BF16),
            bk, dma(()), dma(()), dma((n_local, 2 * len(PARTS) + 3)), bk_sem,
        ],
        compiler_params=pltpu.CompilerParams(vmem_limit_bytes=VMEM_LIMIT),
        name="experts",
    )(info, x, expert_w1, expert_w3, expert_w2)


def fill_kernel(ep, n_local, sc, rnd, e_ref, a_hbm, b_hbm, bk, bk_sem):
    fill_buckets(ep, sc, rnd[0], e_ref, a_hbm, b_hbm, bk, bk_sem, n_local)


def fill_buckets(ep, sc, rnd, e_ref, a_hbm, b_hbm, bk, bk_sem, n_local):
    pc = Place(ep)
    side = pc.side
    slots, dim = e_ref.shape
    width = dim // 4
    pack = 16
    window = (CAP + 2 * pack - 2) // pack * pack
    skip = rnd * CAP

    def out_copies(n):
        dx, dy = lax.rem(n, side), n // side
        targets = [a_hbm.at[dx, c, dy] for c in PAIR] + [b_hbm.at[dy, c, dx] for c in PAIR]
        return [pltpu.make_async_copy(bk.at[n, c], target, bk_sem.at[n, c]) for c, target in enumerate(targets)]

    def one(n):
        dx, dy = lax.rem(n, side), n // side
        chip = lax.rem(pc.py + dy, side) * side + lax.rem(pc.px + dx, side)
        row = iota((CAP, window), 0)
        col = iota((CAP, window), 1)
        out = jnp.zeros((CAP, dim), F32)
        lead = -skip
        for l in range(n_local):
            start, count = sc[2 * l + 1, 2 * chip], sc[2 * l, 2 * chip] + sc[2 * l, 2 * chip + 1]
            used = jnp.minimum(jnp.maximum(-lead, 0), count)
            origin = jnp.minimum((start + used) // pack * pack, slots - window)
            origin = pl.multiple_of(origin, pack)
            slot = row - lead + start
            hit = (slot == col + origin) & (row >= lead) & (row < lead + count)
            out = out + jnp.dot(jnp.where(hit, 1.0, 0.0).astype(BF16), e_ref[pl.ds(origin, window), :], preferred_element_type=F32)
            lead = lead + count
        out = out.astype(BF16)
        for c, copy in enumerate(out_copies(n)):
            bk[n, c] = out[:, c * width : (c + 1) * width]
            copy.start()

    def sent(n):
        for copy in out_copies(n):
            copy.wait()

    loop(side * side, one, unroll=4)
    loop(side * side, sent)


def fill(ep, n_local, info, rnd, e):
    vmem = pl.BlockSpec(memory_space=pltpu.VMEM)
    smem = pl.BlockSpec(memory_space=pltpu.SMEM)
    hbm = pl.BlockSpec(memory_space=pl.ANY)
    bucket = bucket_shape(ep, e.shape[1])
    return pl.pallas_call(
        functools.partial(fill_kernel, ep, n_local),
        out_shape=(bucket, bucket),
        in_specs=[smem, smem, vmem],
        out_specs=(hbm, hbm),
        scratch_shapes=bucket_scratch(ep, e.shape[1]),
        compiler_params=pltpu.CompilerParams(vmem_limit_bytes=VMEM_LIMIT),
        name="fill",
    )(info, rnd, e)


def combine_kernel(
    ep, n_local, a_hbm, b_hbm, q_ref, p_ref, acc_ref, out_ref, bk, st, rl, fin, ry, pf, g_ref, bk_sem, s_send, s_recv, p_send, p_recv
):
    pc = Place(ep)
    side = pc.side
    tok = q_ref.shape[1]
    width = bk.shape[-1]
    loads = [pltpu.make_async_copy(src, bk.at[fam], bk_sem.at[fam]) for fam, src in enumerate((a_hbm, b_hbm))]
    for load in loads:
        load.start()

    barrier = pltpu.get_barrier_semaphore()
    friends = [pc.dev(1, 0), pc.dev(-1, 0), pc.dev(0, 1), pc.dev(0, -1), pc.partner]
    for friend in friends:
        pl.semaphore_signal(barrier, inc=1, device_id={"ep": friend}, device_id_type=MESH)
    pl.semaphore_wait(barrier, len(friends))
    for load in loads:
        load.wait()

    ring = (0, 1, side - 1, 2)

    def held(fam, j):
        return bk.at[fam, 0] if j == 0 else st.at[fam, j]

    def link_copy(fam, g, k):
        hop = 1 if k % 2 == 0 else -1
        c = k % 2
        if g == 0:
            target = pc.at(fam, hop, 0)
            if k < 2:
                src, dst = bk.at[fam, hop % side], st.at[fam, hop % side]
            elif k < 4:
                src, dst = bk.at[fam, 2, c], rl.at[fam, c]
            else:
                src, dst = rl.at[fam, c], st.at[fam, 2, c]
        else:
            j = g - 1
            target = pc.at(fam, 0, hop)
            if k < 2:
                src, dst = held(fam, j).at[:, hop % side], fin.at[fam, j, hop % side]
            elif k < 4:
                src, dst = held(fam, j).at[c, 2], ry.at[fam, j, c]
            else:
                src, dst = ry.at[fam, j, c], fin.at[fam, j, 2, c]
        n = (fam * (side + 1) + g) * 6 + k
        return pltpu.make_async_remote_copy(
            src_ref=src, dst_ref=dst, send_sem=s_send.at[n], recv_sem=s_recv.at[n], device_id={"ep": target}, device_id_type=MESH
        )

    def arrived(fam, j, v):
        return held(fam, j).at[:, 0] if v == 0 else fin.at[fam, j, v]

    def pass_on(fam, j, v):
        n = (fam * side + j) * side + v
        return pltpu.make_async_remote_copy(
            src_ref=arrived(fam, j, v), dst_ref=pf.at[fam, j, v], send_sem=p_send.at[n], recv_sem=p_recv.at[n],
            device_id={"ep": pc.partner}, device_id_type=MESH,
        )

    for k in SENDS:
        for fam in PAIR:
            link_copy(fam, 0, k).start()
    for k in SENDS:
        for fam in PAIR:
            link_copy(fam, 1, k).start()
    for fam in PAIR:
        pass_on(fam, 0, 0).start()

    row = iota((g_ref.shape[3], tok), 0)

    def weights(d):
        w = jnp.zeros(row.shape, F32)
        for l in range(n_local):
            e = d * n_local + l
            w = w + jnp.where(row == q_ref[pl.ds(e, 1), :], p_ref[pl.ds(e, 1), :], 0.0)
        w = w.T
        for n in range(3):
            term = w.astype(BF16)
            g_ref[d, n] = term
            w = w - term.astype(F32)

    loop(ep, weights)
    out_ref[...] = acc_ref[...]

    def add(fam, j, v):
        devs = [pc.at(fam, -j, -v), pc.at(fam, -j, -v, 1 - pc.core)]

        def one(c):
            cols = pl.ds(pl.multiple_of((2 * fam + c) * width, width), width)
            total = out_ref[:, cols]
            for d, rows in zip(devs, (arrived(fam, j, v), pf.at[fam, j, v])):
                data = rows[c]
                for n in range(3):
                    total = total + jnp.dot(g_ref[d, n][:, :CAP], data, preferred_element_type=F32)
            out_ref[:, cols] = total

        loop(2, one, unroll=2)

    ready = []

    def here(fam, j, v):
        pass_on(fam, j, v).start()
        ready.append((fam, j, v))

    def drain(keep):
        while len(ready) > keep:
            fam, j, v = ready.pop(0)
            pass_on(fam, j, v).wait_recv()
            add(fam, j, v)

    def got(fam, g, k):
        link_copy(fam, g, k).wait_recv()

    ready += [(0, 0, 0), (1, 0, 0)]
    for k in SPLIT:
        for fam in PAIR:
            got(fam, 0, k)
            link_copy(fam, 0, k + 2).start()
    drain(0)
    for k in PAIR:
        for fam in PAIR:
            got(fam, 0, k)
            j = 1 if k == 0 else side - 1
            for kk in SENDS:
                link_copy(fam, 1 + j, kk).start()
            here(fam, j, 0)
    for k in SPLIT:
        for fam in PAIR:
            got(fam, 1, k)
            link_copy(fam, 1, k + 2).start()
    for fam in PAIR:
        got(fam, 0, 4)
        got(fam, 0, 5)
        for kk in SENDS:
            link_copy(fam, 3, kk).start()
        here(fam, 2, 0)
    drain(2)
    for j in ring:
        if j > 0:
            for k in SPLIT:
                for fam in PAIR:
                    got(fam, 1 + j, k)
                    link_copy(fam, 1 + j, k + 2).start()
        for k in PAIR:
            for fam in PAIR:
                got(fam, 1 + j, k)
                here(fam, j, 1 if k == 0 else side - 1)
        drain(2)
    for j in ring:
        for fam in PAIR:
            got(fam, 1 + j, 4)
            got(fam, 1 + j, 5)
            here(fam, j, 2)
        drain(4)
    drain(0)
    for fam in PAIR:
        for g in range(side + 1):
            for k in range(6):
                link_copy(fam, g, k).wait_send()
        for j in range(side):
            for v in range(side):
                pass_on(fam, j, v).wait_send()


def combine(ep, n_local, bka, bkb, q, weights, acc):
    side = math.isqrt(ep // 2)
    cap, width = bka.shape[-2:]
    tok = q.shape[1]
    vmem = pl.BlockSpec(memory_space=pltpu.VMEM)
    hbm = pl.BlockSpec(memory_space=pl.ANY)
    dma = pltpu.SemaphoreType.DMA
    n_link, n_pass = 2 * (side + 1) * 6, 2 * side * side
    return pl.pallas_call(
        functools.partial(combine_kernel, ep, n_local),
        out_shape=jax.ShapeDtypeStruct(acc.shape, F32),
        in_specs=[hbm, hbm, vmem, vmem, vmem],
        out_specs=vmem,
        scratch_shapes=[
            pltpu.VMEM((2, side, 2, side, cap, width), BF16),
            pltpu.VMEM((2, side, 2, side, cap, width), BF16),
            pltpu.VMEM((2, 2, side, cap, width), BF16),
            pltpu.VMEM((2, side, side, 2, cap, width), BF16),
            pltpu.VMEM((2, side, 2, cap, width), BF16),
            pltpu.VMEM((2, side, side, 2, cap, width), BF16),
            pltpu.VMEM((ep, 3, tok, tok), BF16),
            dma((2,)), dma((n_link,)), dma((n_link,)), dma((n_pass,)), dma((n_pass,)),
        ],
        compiler_params=pltpu.CompilerParams(collective_id=1, has_side_effects=True, vmem_limit_bytes=VMEM_LIMIT),
        name="combine",
    )(bka, bkb, q, weights, acc)


def solution(mesh):
    ep = mesh.shape["ep"]
    tok_spec = P(("dp", "ep"))
    expert_spec = P("ep")

    def device_fn(resid_in, expert_ids, priority, norm_gain, router_w, shared_w1, shared_w3, shared_w2, expert_w1, expert_w3, expert_w2):
        n_local = expert_w1.shape[0]
        x, info, q, gates, base = dispatch(
            ep, n_local, resid_in, expert_ids, priority, norm_gain, router_w, shared_w1, shared_w3, shared_w2
        )
        e, bka, bkb = experts(ep, info, x, expert_w1, expert_w3, expert_w2)
        first = combine(ep, n_local, bka, bkb, q, gates, base)
        rounds = lax.div(info[2 * n_local, 0] + (CAP - 1), CAP)

        def one_round(carry):
            rnd, acc = carry
            more_a, more_b = fill(ep, n_local, info, rnd[None], e)
            return rnd + 1, combine(ep, n_local, more_a, more_b, q - rnd * CAP, gates, acc)

        total = lax.while_loop(lambda carry: carry[0] < rounds, one_round, (jnp.int32(1), first))[1]
        return total.astype(BF16)

    return jax.shard_map(
        device_fn, mesh=mesh,
        in_specs=(tok_spec, tok_spec, tok_spec, P(), P(), P(), P(), P(), expert_spec, expert_spec, expert_spec),
        out_specs=tok_spec, check_vma=False,
    )
```
